256 devices in a mesh: freq: 4 (over x_hi, core), rcv: 64 (over y, z, x_lo).
Axes of the slice: x: 4 (x_hi: 2, x_lo: 2; x = x_hi * 2 + x_lo), y: 4, z: 8, core: 2. Of those that a mesh axis runs over, the one named last changes fastest.
Arguments:
- reflection: bfloat16 [8, 2, 2560, 2560], P('freq', None, 'rcv'), may hold values from -5 to 5, as said below
- starts: int32 [2560, 192], P('rcv'), may hold values from 8 to 56
- focusing: float32 [8, 2560, 2, 192], P('freq', 'rcv'), may hold values from -6 to 6
- residual: float32 [8, 2560, 2, 192], P('freq', 'rcv'), may hold values from -6 to 6
- direction: float32 [8, 2560, 2, 192], P('freq', 'rcv'), may hold values from -6 to 6
- gradient: float32 [8, 2560, 2, 192], P('freq', 'rcv'), may hold values from -30 to 30
Outputs:
- new_focusing: float32 [8, 2560, 2, 192], P('freq', 'rcv')
- new_residual: float32 [8, 2560, 2, 192], P('freq', 'rcv')
- new_direction: float32 [8, 2560, 2, 192], P('freq', 'rcv')
- green_field: float32 [8, 2560, 2, 192], P('freq', 'rcv')
- focal_correlation: float32 [8, 2, 192], P('freq')
The draws below stay inside these ranges and needn't reach their ends.
Inputs may be any that keep to these rules, and one draw needn't show every extreme that they name: Each frequency's matrix is symmetric in source and receiver: reflection[f, c, s, r] = reflection[f, c, r, s].
All inputs are finite; a program needn't handle non-finite values.
Results may differ from the reference program's by a relative error of at most 0.0003.
The reference program's roundings to bfloat16 on the way (of `gated`) count: a program that leaves them out, or rounds other values in their place, can miss the bound.
Values may be sent and summed in bfloat16 or wider, within the bound.
A program may use at most 64 MiB of HBM per device.

```python
import math
import jax
import jax.numpy as jnp
from jax import lax

N = 2560
K = 192
F = 8
TS = 64


def rising(count):
    position = jnp.arange(count, dtype=jnp.float32)
    return 3.0 ** (position / max(count - 1, 1) - 0.5)


def draw_reflection(key, part):
    row_scale = rising(N)
    freq_scale = rising(F)

    def single(position):
        noise = jnp.clip(jax.random.normal(jax.random.fold_in(key, position), (2, N, N), jnp.float32), -6.0, 6.0)
        symmetric = (noise + jnp.transpose(noise, (0, 2, 1))) * (0.5 / math.sqrt(N))
        scaled = symmetric * row_scale[:, None] * row_scale[None, :] * freq_scale[position]
        return scaled.astype(jnp.bfloat16)
    return lax.map(single, jnp.arange(F, dtype=jnp.int32))


def draw_gradient(key, part):
    noise = jnp.clip(jax.random.normal(key, (F, N, 2, K), jnp.float32), -6.0, 6.0) * 0.5
    row_scale = rising(N)
    scale = rising(F)[:, None, None, None] * row_scale[None, :, None, None]
    return noise * scale


def with_ends(values, rng, low, high):
    longest = values.shape.index(max(values.shape))
    spots = []
    for shift in (0, 1):
        where = [jax.random.randint(jax.random.fold_in(rng, axis), (), 0, length) for axis, length in enumerate(values.shape)]
        where[longest] = (where[longest] + shift) % values.shape[longest]
        spots.append(tuple(where))
    return values.at[spots[0]].set(low).at[spots[1]].set(high)


def levels(stream_key, extent, split, least, largest):
    loudness = 1.0
    for dim, shards_of in split:
        draws = jax.random.uniform(jax.random.fold_in(jax.random.fold_in(stream_key, 6), dim), (shards_of,), jnp.float32, least / len(split), largest / len(split))
        loudness = loudness * jnp.repeat(jnp.exp(draws), extent[dim] // shards_of).reshape((-1,) + (1,) * (len(extent) - 1 - dim))
    return loudness


def normal_values(key, extent, width, bound, shards=(), held_as=jnp.bfloat16):
    result = width * jax.random.normal(key, extent, jnp.float32)
    if shards:
        result = result * levels(key, extent, shards, -0.22, 0.18)
    return jnp.clip(result, -bound, bound).astype(held_as)


def setup_inputs(seed: int = 0) -> dict:
    splits = jax.random.split(jax.random.key(seed), 7)
    return {
        "reflection": draw_reflection(jax.random.fold_in(splits[6], 71), 0),
        "starts": with_ends(jax.random.randint(splits[1], (N, K), TS // 8, TS - TS // 8 + 1), jax.random.fold_in(splits[1], 1), TS // 8, (TS - TS // 8 + 1) - 1).astype(jnp.int32),
        "focusing": normal_values(splits[2], (F, N, 2, K), 1.0, 6.0, ((0, 4), (1, 64)), jnp.float32),
        "residual": normal_values(splits[3], (F, N, 2, K), 1.0, 6.0, ((0, 4), (1, 64)), jnp.float32),
        "direction": normal_values(splits[4], (F, N, 2, K), 1.0, 6.0, ((0, 4), (1, 64)), jnp.float32),
        "gradient": draw_gradient(jax.random.fold_in(splits[6], 71), 0),
    }


band_start = 5
tiny = 1e-06
highest = lax.Precision.HIGHEST

def tables(count, offset):
    times = jnp.arange(TS, dtype=jnp.float32)[:, None]
    bins = (jnp.arange(count, dtype=jnp.int32) + offset + band_start).astype(jnp.float32)[None, :]
    phase = 2.0 * jnp.pi * times * bins / TS
    return (jnp.cos(phase), jnp.sin(phase))

def contract_time(table, values):
    return jnp.einsum('tf,frk->trk', table, values, precision=highest)

def contract_back(table, values):
    return jnp.einsum('tf,trk->frk', table, values, precision=highest)

def time_gate(field, forward_cos, forward_sin, back_cos, back_sin, limits, complement):
    real_part = field[:, :, 0]
    imag_part = field[:, :, 1]
    time_real = contract_time(forward_cos, real_part) - contract_time(forward_sin, imag_part)
    time_imag = contract_time(forward_sin, real_part) + contract_time(forward_cos, imag_part)
    clock = jnp.arange(TS, dtype=jnp.int32)[:, None, None]
    window = (clock < limits[None]).astype(jnp.float32)
    if complement:
        window = 1.0 - window
    kept_real = window * time_real
    kept_imag = window * time_imag
    out_real = (contract_back(back_cos, kept_real) + contract_back(back_sin, kept_imag)) / TS
    out_imag = (contract_back(back_cos, kept_imag) - contract_back(back_sin, kept_real)) / TS
    return jnp.stack([out_real, out_imag], axis=2)

def product(left, right):
    return jnp.dot(left, right, preferred_element_type=jnp.float32)

def forward_apply(reflection, values):

    def single(pair):
        matrix, vector = pair
        out_real = product(matrix[0], vector[:, 0]) - product(matrix[1], vector[:, 1])
        out_imag = product(matrix[0], vector[:, 1]) + product(matrix[1], vector[:, 0])
        return jnp.stack([out_real, out_imag], axis=1)
    return lax.map(single, (reflection, values))

def adjoint_apply(reflection, values):

    def single(pair):
        matrix, vector = pair
        real_t = matrix[0].T
        imag_t = matrix[1].T
        out_real = product(real_t, vector[:, 0]) + product(imag_t, vector[:, 1])
        out_imag = product(real_t, vector[:, 1]) - product(imag_t, vector[:, 0])
        return jnp.stack([out_real, out_imag], axis=1)
    return lax.map(single, (reflection, values))

def reference(reflection, starts, focusing, residual, direction, gradient):
    cos_table, sin_table = tables(F, 0)

    def gate(field, complement):
        return time_gate(field, cos_table, sin_table, cos_table, sin_table, starts, complement)
    direction_image = forward_apply(reflection, direction.astype(jnp.bfloat16))
    focusing_image = forward_apply(reflection, focusing.astype(jnp.bfloat16))
    image = gate(direction_image, False)
    gamma = jnp.sum(gradient * gradient)
    curvature = jnp.sum(image * image)
    alpha = gamma / (curvature + tiny)
    new_focusing = focusing + alpha * direction
    new_residual = residual - alpha * image
    gated = gate(new_residual, False).astype(jnp.bfloat16)
    new_gradient = adjoint_apply(reflection, gated)
    new_gamma = jnp.sum(new_gradient * new_gradient)
    new_direction = new_gradient + new_gamma / (gamma + tiny) * direction
    green_field = gate(focusing_image + alpha * direction_image, True)
    corr_real = lax.optimization_barrier(jnp.sum(green_field[:, :, 0] * new_focusing[:, :, 0] + green_field[:, :, 1] * new_focusing[:, :, 1], axis=1))
    corr_imag = lax.optimization_barrier(jnp.sum(green_field[:, :, 1] * new_focusing[:, :, 0] - green_field[:, :, 0] * new_focusing[:, :, 1], axis=1))
    focal_correlation = jnp.stack([corr_real, corr_imag], axis=1) / math.sqrt(N)
    return (new_focusing, new_residual, new_direction, green_field, focal_correlation)
```

```python
import math

import jax
import jax.numpy as jnp
from jax import lax
from jax.sharding import Mesh
from jax.sharding import PartitionSpec as P

N = 2560
F = 8
TS = 64
FREQ = ("freq_0", "freq_1")
RCV = ("rcv_0", "rcv_1", "rcv_2")
FREQ_RCV = ("freq_0", "freq_1", "rcv_0", "rcv_1", "rcv_2")


band_start = 5
tiny = 1e-06
highest = lax.Precision.HIGHEST


def in_order(pieces, dim):
    lengths = list(pieces.shape[1:])
    lengths[dim] *= pieces.shape[0]
    return jnp.moveaxis(pieces, 0, dim).reshape(lengths)


def sent_to_all(value, axis):
    count = lax.axis_size(axis)
    return lax.all_to_all(
        jnp.broadcast_to(value[None], (count, *value.shape)), axis, 0, 0, tiled=True
    )


def gather_directly(value, axis, dim):
    return in_order(sent_to_all(value, axis), dim)


def one_axis_at_a_time(value, axes):
    for axis in axes:
        value = lax.psum(value, axis)
    return value


def all_blocks(value, axes, sequence):
    pieces = value
    for k in sequence:
        pieces = lax.all_gather(pieces, axes[k])
    done = sequence[::-1]
    back = [done.index(k) for k in range(len(axes))]
    pieces = pieces.transpose(*back, *range(len(axes), pieces.ndim))
    return pieces.reshape(-1, *value.shape)


def gathered_by_axis(value, axes, sequence, dim):
    return in_order(all_blocks(value, axes, sequence), dim)


def of_everyone(value, axis):
    everything = sent_to_all(value, axis)
    return jnp.sum(everything, axis=0)


def tables(count, offset):
    times = jnp.arange(TS, dtype=jnp.float32)[:, None]
    bins = (jnp.arange(count, dtype=jnp.int32) + offset + band_start).astype(jnp.float32)[None, :]
    phase = 2.0 * jnp.pi * times * bins / TS
    return (jnp.cos(phase), jnp.sin(phase))


def contract_time(table, values):
    return jnp.einsum("tf,frk->trk", table, values, precision=highest)


def contract_back(table, values):
    return jnp.einsum("tf,trk->frk", table, values, precision=highest)


def time_gate(field, forward_cos, forward_sin, back_cos, back_sin, limits, complement):
    real_part = field[:, :, 0]
    imag_part = field[:, :, 1]
    time_real = contract_time(forward_cos, real_part) - contract_time(forward_sin, imag_part)
    time_imag = contract_time(forward_sin, real_part) + contract_time(forward_cos, imag_part)
    clock = jnp.arange(TS, dtype=jnp.int32)[:, None, None]
    window = (clock < limits[None]).astype(jnp.float32)
    if complement:
        window = 1.0 - window
    kept_real = window * time_real
    kept_imag = window * time_imag
    out_real = (contract_back(back_cos, kept_real) + contract_back(back_sin, kept_imag)) / TS
    out_imag = (contract_back(back_cos, kept_imag) - contract_back(back_sin, kept_real)) / TS
    return jnp.stack([out_real, out_imag], axis=2)


def combine(total, conjugate):
    if conjugate:
        out_real = total[:, 0, :, 0] + total[:, 1, :, 1]
        out_imag = total[:, 0, :, 1] - total[:, 1, :, 0]
    else:
        out_real = total[:, 0, :, 0] - total[:, 1, :, 1]
        out_imag = total[:, 0, :, 1] + total[:, 1, :, 0]
    return jnp.stack([out_real, out_imag], axis=2)


def per_device(reflection, starts, focusing, residual, direction, gradient):
    local_freq = reflection.shape[0]
    position = lax.axis_index(FREQ)
    cos_table, sin_table = tables(F, 0)
    own_cos, own_sin = tables(local_freq, position * local_freq)

    def gate(field, complement):
        whole = gather_directly(field, FREQ, 0)
        return time_gate(whole, cos_table, sin_table, own_cos, own_sin, starts, complement)

    def accumulate(piece):
        return jnp.einsum("fpnm,fmqk->fpnqk", reflection, piece, preferred_element_type=jnp.float32)

    direction_low = direction.astype(jnp.bfloat16)
    focusing_low = focusing.astype(jnp.bfloat16)
    aimed_total = accumulate(gathered_by_axis(direction_low, RCV, (2, 0, 1), 1))
    direction_image = combine(aimed_total, False)
    image = gate(direction_image, False)
    gamma, curvature = (
        one_axis_at_a_time(jnp.sum(gradient * gradient), FREQ_RCV),
        one_axis_at_a_time(jnp.sum(image * image), FREQ_RCV),
    )
    alpha = gamma / (curvature + tiny)
    new_focusing = focusing + alpha * direction
    new_residual = residual - alpha * image
    gated = gate(new_residual, False).astype(jnp.bfloat16)
    total = accumulate(gathered_by_axis(gated, RCV, (2, 0, 1), 1))
    new_gradient = combine(total, True)
    new_gamma = one_axis_at_a_time(jnp.sum(new_gradient * new_gradient), FREQ_RCV)
    new_direction = new_gradient + new_gamma / (gamma + tiny) * direction
    focus_total = accumulate(gathered_by_axis(focusing_low, RCV, (2, 0, 1), 1))
    focusing_image = combine(focus_total, False)
    green_field = gate(focusing_image + alpha * direction_image, True)
    corr_real = jnp.sum(
        green_field[:, :, 0] * new_focusing[:, :, 0] + green_field[:, :, 1] * new_focusing[:, :, 1],
        axis=1,
    )
    corr_imag = jnp.sum(
        green_field[:, :, 1] * new_focusing[:, :, 0] - green_field[:, :, 0] * new_focusing[:, :, 1],
        axis=1,
    )
    partial_corr = jnp.stack([corr_real, corr_imag], axis=1)
    focal_correlation = of_everyone(partial_corr, RCV) / math.sqrt(N)
    return (new_focusing, new_residual, new_direction, green_field, focal_correlation)


def solution(mesh):
    finer = Mesh(
        mesh.devices.reshape(2, 2, 4, 8, 2), ("freq_0", "freq_1", "rcv_0", "rcv_1", "rcv_2")
    )
    in_specs = (
        P(FREQ, None, RCV, None),
        P(RCV, None),
        P(FREQ, RCV, None, None),
        P(FREQ, RCV, None, None),
        P(FREQ, RCV, None, None),
        P(FREQ, RCV, None, None),
    )
    out_specs = (
        P(FREQ, RCV, None, None),
        P(FREQ, RCV, None, None),
        P(FREQ, RCV, None, None),
        P(FREQ, RCV, None, None),
        P(FREQ, None, None),
    )
    return jax.shard_map(
        per_device, mesh=finer, in_specs=in_specs, out_specs=out_specs, check_vma=False
    )
```

```python
import cmath
import functools
import math

import jax
import jax.numpy as jnp
from jax import lax
from jax.experimental import pallas as pl
from jax.experimental.pallas import tpu as pltpu
from jax.sharding import Mesh
from jax.sharding import PartitionSpec as P

N = 2560
K = 192
F = 8
TS = 64
ROWS = 40
W = 2 * K
COLS = 640
TINY = 1e-06
AXES = ("freq_0", "freq_1", "rcv_0", "rcv_1", "rcv_2")
FREQ = AXES[:2]
RCV = AXES[2:]
MESH = pl.DeviceIdType.MESH
BF = jnp.bfloat16
F32 = jnp.float32


def swap(x):
    return jnp.concatenate([x[:, K:], x[:, :K]], axis=1)


def kernel(
    refl, starts, foc, res, dirn, grad,
    o_foc, o_res, o_dir, o_green, o_corr,
    gb, rbuf, rbig, rtmp, vtmp, acc, part, rs, fx, ta, tb, img, tr, ti, arb, cb,
    g_send, g_recv, x_send, x_recv, r_send, r_recv, s_send, s_recv, f_send, f_recv,
    a_send, a_recv, c_send, c_recv,
):
    xh, c, y, z, xl = (lax.axis_index(a) for a in AXES)
    q = xh * 2 + c
    pending = []

    def dev(**other):
        me = {"xh": xh, "c": c, "y": y, "z": z, "xl": xl}
        me.update(other)
        return tuple(me[n] for n in ("xh", "c", "y", "z", "xl"))

    def copy(src, dst, ss, rr, to):
        return pltpu.make_async_remote_copy(
            src_ref=src, dst_ref=dst, send_sem=ss, recv_sem=rr, device_id=to, device_id_type=MESH
        )

    def start(*args):
        d = copy(*args)
        d.start()
        pending.append(d)

    cell = []
    for i in range(1, 8):
        dx, dc, dl = i >> 2, (i >> 1) & 1, i & 1
        cell.append(((xh + dx) % 2, (c + dc) % 2, (xl + dl) % 2))
    cell_peers = [(dev(xh=a, c=b, xl=d), a * 4 + b * 2 + d) for a, b, d in cell]
    y_peers = [(dev(y=(y + i) % 4), (y + i) % 4) for i in (2, 1, 3)]
    z_peers = [(dev(z=(z + i) % 8), (z + i) % 8) for i in range(1, 8)]
    x_peer = dev(xl=1 - xl)

    for f in range(2):
        gb[0, f, z, xl] = dirn[f].astype(BF)
        gb[1, f, z, xl] = foc[f].astype(BF)

    barrier = pltpu.get_barrier_semaphore()
    everyone = [p for p, _ in cell_peers + y_peers + z_peers]
    for p in everyone:
        pl.semaphore_signal(barrier, inc=1, device_id=p, device_id_type=MESH)
    pl.semaphore_wait(barrier, len(everyone))

    order = [(0, 0), (1, 0), (0, 1), (1, 1)]

    def valid(s, way, f):
        return s < 4 or f == way

    def unit(k, f, a, zz):
        return gb.at[k, f, zz, xl if a == 0 else 1 - xl]

    def gsem(way, s, f, a):
        return ((way * 4 + s - 1) * 2 + f) * 2 + a

    seen = set()

    def wait_unit(k, way, s, f, a):
        if (k, way, s, f, a) in seen:
            return
        seen.add((k, way, s, f, a))
        zz = (z - s + 8) % 8 if way == 0 else (z + s) % 8
        u = unit(k, f, a, zz)
        i = gsem(way, s, f, a)
        copy(u, u, g_send.at[k, i], g_recv.at[k, i], x_peer).wait_recv()

    def exchange(k):
        for f in range(2):
            u = gb.at[k, f, z, xl]
            start(u, u, x_send.at[k, f], x_recv.at[k, f], x_peer)

    def ring(k, s, sides=(0, 1)):
        for f, a in order:
            if a not in sides:
                continue
            if s == 1 and a == 1:
                u = gb.at[k, f, z, 1 - xl]
                copy(u, u, x_send.at[k, f], x_recv.at[k, f], x_peer).wait_recv()
            for way in range(2):
                if not valid(s, way, f):
                    continue
                if s > 1:
                    wait_unit(k, way, s - 1, f, a)
                zz = (z - s + 9) % 8 if way == 0 else (z + s - 1) % 8
                to = dev(z=(z + 1) % 8 if way == 0 else (z + 7) % 8)
                u = unit(k, f, a, zz)
                i = gsem(way, s, f, a)
                start(u, u, g_send.at[k, i], g_recv.at[k, i], to)

    def gathered(k):
        for s in range(1, 5):
            for f, a in order:
                for way in range(2):
                    if valid(s, way, f):
                        wait_unit(k, way, s, f, a)

    lane = lax.broadcasted_iota(jnp.int32, (8, W), 1)
    sign = jnp.where(lane < K, -1.0, 1.0).astype(F32)
    sign_rows = jnp.where(
        lax.broadcasted_iota(jnp.int32, (ROWS, W), 1) < K, -1.0, 1.0
    ).astype(F32)

    def send_reflection():
        for i, (p, yy) in enumerate(y_peers):
            cols = pl.ds(pl.multiple_of(yy * COLS, 128), COLS)
            start(refl.at[:, :, :, cols], rbuf.at[y], r_send.at[i], r_recv.at[i], p)

    def assemble_reflection():
        cols = pl.ds(pl.multiple_of(y * COLS, 128), COLS)
        for f in range(2):
            for p in range(2):
                rbuf[y, f, p] = refl[f, p, :, cols]
        for i, j in enumerate((2, 3, 1)):
            src = rbuf.at[(y + j) % 4]
            copy(src, src, r_send.at[i], r_recv.at[i], x_peer).wait_recv()
        for f in range(2):

            def put(i, _, f=f):
                rows = pl.ds(pl.multiple_of(i * ROWS, 8), ROWS)
                rtmp[rows, :] = rbuf[i // 2, f, i % 2].astype(F32)
                return 0

            lax.fori_loop(0, 8, put, 0)
            rbig[f] = rtmp[...].astype(BF)

    def multiply(k, conjugate):
        for f in range(2):

            def put(i, _, f=f):
                rows = pl.ds(pl.multiple_of(i * ROWS, 8), ROWS)
                vtmp[rows, :] = gb[k, f, i // 2, i % 2].astype(F32)
                return 0

            lax.fori_loop(0, 16, put, 0)
            acc[...] = jnp.dot(rbig[f], vtmp[...].astype(BF), preferred_element_type=F32)
            for i, (p, yy) in enumerate(y_peers + [(None, y)]):
                first = acc[pl.ds(pl.multiple_of(yy * 80, 8), ROWS), :]
                second = acc[pl.ds(pl.multiple_of(yy * 80 + 40, 8), ROWS), :]
                turned = sign_rows * swap(second)
                part[k, i, f] = first - turned if conjugate else first + turned
                if p is not None:
                    start(part.at[k, i, f], rs.at[k, y, f], s_send.at[k, i, f], s_recv.at[k, i, f], p)

    def reduced(k, f):
        total = part[k, 3, f]
        for i, j in enumerate((2, 3, 1)):
            src = rs.at[k, (y + j) % 4, f]
            copy(src, src, s_send.at[k, i, f], s_recv.at[k, i, f], x_peer).wait_recv()
            total = total + rs[k, (y + j) % 4, f]
        return total

    q_c = xh * 2 + 1 - c
    q_x = (1 - xh) * 2 + c
    q_xc = (1 - xh) * 2 + 1 - c

    def share(k):
        u = fx.at[k, q]
        start(u, u, f_send.at[k, 1], f_recv.at[k, 1], dev(xh=1 - xh))
        start(u, u, f_send.at[k, 0], f_recv.at[k, 0], dev(c=1 - c))

    def relay(k):
        u = fx.at[k, q_x]
        copy(u, u, f_send.at[k, 1], f_recv.at[k, 1], x_peer).wait_recv()
        start(u, u, f_send.at[k, 2], f_recv.at[k, 2], dev(c=1 - c))

    def shared(k):
        for i, qq in ((0, q_c), (2, q_xc)):
            u = fx.at[k, qq]
            copy(u, u, f_send.at[k, i], f_recv.at[k, i], x_peer).wait_recv()

    def band(r):
        return pl.ds(pl.multiple_of(r * 8, 8), 8)

    def tables():
        def one(r, _):
            rows = band(r)
            s = jnp.clip(starts[rows, :], 0, TS)
            zr = jnp.ones((8, W), F32)
            zi = jnp.zeros((8, W), F32)
            for b in range(6):
                w = cmath.exp(2j * math.pi * (1 << b) / TS)
                on = (s & (1 << b)) != 0
                nr, ni = zr * w.real - zi * w.imag, zr * w.imag + zi * w.real
                zr, zi = jnp.where(on, nr, zr), jnp.where(on, ni, zi)
            ta[7, rows, :] = s.astype(F32) * (1.0 / TS)
            tb[7, rows, :] = jnp.zeros((8, W), F32)
            pr, pi = zr, zi
            for d in range(1, 8):
                k = 1.0 / (TS * (1.0 - cmath.exp(2j * math.pi * d / TS)))
                gr = k.real - (k.real * pr - k.imag * pi)
                gi = sign * (k.imag - (k.real * pi + k.imag * pr))
                ta[7 + d, rows, :] = gr
                ta[7 - d, rows, :] = gr
                tb[7 + d, rows, :] = gi
                tb[7 - d, rows, :] = -gi
                pr, pi = pr * zr - pi * zi, pr * zi + pi * zr
            return 0

        lax.fori_loop(0, ROWS // 8, one, 0)

    def gate_own(fields, e, rows):
        total = None
        for j, (u, v) in enumerate(fields):
            d = 7 + j - e - 2 * q
            term = ta[d, rows, :] * u + tb[d, rows, :] * v
            total = term if total is None else total + term
        return total

    def fields_of(k, rows):
        us = [fx[k, j // 2, j % 2, rows, :] for j in range(F)]
        return [(u, swap(u)) for u in us]

    def gate_residual():
        def one(r, _):
            rows = band(r)
            fields = fields_of(0, rows)
            for e in range(2):
                tr[e, rows, :] = gate_own(fields, e, rows)
            return 0

        lax.fori_loop(0, ROWS // 8, one, 0)

    def gate_image():
        def one(r, total):
            rows = band(r)
            fields = fields_of(1, rows)
            images = []
            for j in range(F):
                t = ta[7, rows, :] * fields[j][0]
                for i in range(F):
                    if i != j:
                        d = 7 + i - j
                        t = t + ta[d, rows, :] * fields[i][0] + tb[d, rows, :] * fields[i][1]
                img[j, rows, :] = t
                images.append((t, swap(t)))
                total = total + t * t
            for e in range(2):
                ti[e, rows, :] = gate_own(images, e, rows)
            return total

        return lax.fori_loop(0, ROWS // 8, one, jnp.zeros((8, W), F32))

    def squares(load):
        def one(r, total):
            for e in range(2):
                x = load(e, band(r))
                total = total + x * x
            return total

        return lax.fori_loop(0, ROWS // 8, one, jnp.zeros((8, W), F32))

    def added(x):
        x = jnp.sum(x, axis=0, keepdims=True)
        return jnp.sum(x, axis=1, keepdims=True)

    cell_slot = xh * 4 + c * 2 + xl

    def put_sum(buf, ss, rr, slot, peers, value):
        buf[slot] = value
        for i, (p, _) in enumerate(peers):
            start(buf.at[slot], buf.at[slot], ss.at[i], rr.at[i], p)

    def get_sum(buf, ss, rr, peers, back, count):
        for i, j in enumerate(back):
            u = buf.at[j]
            copy(u, u, ss.at[i], rr.at[i], x_peer).wait_recv()
        total = buf[0]
        for i in range(1, count):
            total = total + buf[i]
        return total

    cell_back = [s for _, s in cell_peers]
    y_back = [(y + j) % 4 for j in (2, 3, 1)]
    z_back = [(z + 8 - i) % 8 for i in range(1, 8)]
    phases = [(cell_slot, cell_peers, cell_back, 8), (y, y_peers, y_back, 4), (z, z_peers, z_back, 8)]

    def sum_put(k, phase, value):
        slot, peers, _, _ = phases[phase]
        put_sum(arb.at[k, phase], a_send.at[k, phase], a_recv.at[k, phase], slot, peers, value)

    def sum_get(k, phase):
        _, peers, back, count = phases[phase]
        return get_sum(arb.at[k, phase], a_send.at[k, phase], a_recv.at[k, phase], peers, back, count)

    corr_phases = [(xl, [(x_peer, 1 - xl)], [1 - xl], 2), (y, y_peers, y_back, 4), (z, z_peers, z_back, 8)]

    def corr_put(phase, value):
        slot, peers, _, _ = corr_phases[phase]
        put_sum(cb.at[phase], c_send.at[phase], c_recv.at[phase], slot, peers, value)

    def corr_get(phase):
        _, peers, back, count = corr_phases[phase]
        return get_sum(cb.at[phase], c_send.at[phase], c_recv.at[phase], peers, back, count)

    exchange(0)
    ring(0, 1, (0,))
    send_reflection()
    fx[0, q] = res[...]
    ring(0, 1, (1,))
    exchange(1)
    share(0)
    ring(0, 2)
    tables()
    gamma_own = added(squares(lambda e, rows: grad[e, rows, :]))
    ring(0, 3)
    assemble_reflection()
    ring(0, 4)
    ring(1, 1)
    relay(0)
    gathered(0)
    multiply(0, False)
    ring(1, 2)
    for f in range(2):
        fx[1, q, f] = reduced(0, f)
    share(1)
    ring(1, 3)
    shared(0)
    gate_residual()
    relay(1)
    shared(1)
    curvature_own = added(gate_image()) * 0.25
    half = lax.broadcasted_iota(jnp.int32, (1, 128), 1) < 64
    sum_put(0, 0, jnp.where(half, gamma_own, curvature_own))
    ring(1, 4)
    sum_put(0, 1, sum_get(0, 0))
    gathered(1)
    sum_put(0, 2, sum_get(0, 1))
    both = sum_get(0, 2)
    gamma, curvature = both[:, 0:1], both[:, 64:65]
    alpha = gamma / (curvature + TINY)
    for f in range(2):
        gb[2, f, z, xl] = (tr[f] - alpha * ti[f]).astype(BF)
    exchange(2)
    ring(2, 1, (0,))
    multiply(1, False)
    ring(2, 1, (1,))
    for f in range(2):
        o_foc[f] = foc[f] + alpha * dirn[f]
        o_res[f] = res[f] - alpha * img[2 * q + f]
    ring(2, 2)
    for f in range(2):
        fx[2, q, f] = reduced(1, f)
    share(2)
    ring(2, 3)
    relay(2)
    ring(2, 4)
    shared(2)

    def green(r, total):
        rows = band(r)
        fields = fields_of(2, rows)
        out = []
        for e in range(2):
            own = fx[2, q, e, rows, :]
            g = own - gate_own(fields, e, rows)
            g = g + alpha * (fx[1, q, e, rows, :] - img[2 * q + e, rows, :])
            o_green[e, rows, :] = g
            v = o_foc[e, rows, :]
            out += [total[2 * e] + g * v, total[2 * e + 1] + g * swap(v)]
        return tuple(out)

    def finish_corr():
        none = jnp.zeros((8, W), F32)
        sums = lax.fori_loop(0, ROWS // 8, green, (none, none, none, none))
        out = []
        for e in range(2):
            a = jnp.sum(sums[2 * e], axis=0, keepdims=True)
            b = jnp.sum(sums[2 * e + 1], axis=0, keepdims=True)
            out.append(jnp.where(lane[:1] < K, a + swap(a), b - swap(b)))
        return jnp.concatenate(out, axis=0)

    gathered(2)
    multiply(2, True)
    corr_put(0, finish_corr())
    for f in range(2):
        o_dir[f] = reduced(2, f)
    sum_put(1, 0, jnp.broadcast_to(added(squares(lambda e, rows: o_dir[e, rows, :])), (1, 128)))
    corr_put(1, corr_get(0))
    sum_put(1, 1, sum_get(1, 0))
    corr_put(2, corr_get(1))
    sum_put(1, 2, sum_get(1, 1))
    o_corr[...] = corr_get(2) * (1.0 / math.sqrt(N))
    new_gamma = sum_get(1, 2)[:, 0:1]
    ratio = new_gamma / (gamma + TINY)
    for f in range(2):
        o_dir[f] = o_dir[f] + ratio * dirn[f]
    for d in pending:
        d.wait_send()


def per_device(reflection, starts, focusing, residual, direction, gradient):
    def flat(v):
        return v.reshape(2, ROWS, W)

    field = jax.ShapeDtypeStruct((2, ROWS, W), F32)
    dma = pltpu.SemaphoreType.DMA
    vmem = pl.BlockSpec(memory_space=pltpu.VMEM)
    outs = pl.pallas_call(
        kernel,
        out_shape=(field, field, field, field, jax.ShapeDtypeStruct((2, W), F32)),
        in_specs=[vmem] * 6,
        out_specs=[vmem] * 5,
        scratch_shapes=[
            pltpu.VMEM((3, 2, 8, 2, ROWS, W), BF),
            pltpu.VMEM((4, 2, 2, ROWS, COLS), BF),
            pltpu.VMEM((2, 320, COLS), BF),
            pltpu.VMEM((320, COLS), F32),
            pltpu.VMEM((COLS, W), F32),
            pltpu.VMEM((320, W), F32),
            pltpu.VMEM((3, 4, 2, ROWS, W), F32),
            pltpu.VMEM((3, 4, 2, ROWS, W), F32),
            pltpu.VMEM((3, 4, 2, ROWS, W), F32),
            pltpu.VMEM((15, ROWS, W), F32),
            pltpu.VMEM((15, ROWS, W), F32),
            pltpu.VMEM((F, ROWS, W), F32),
            pltpu.VMEM((2, ROWS, W), F32),
            pltpu.VMEM((2, ROWS, W), F32),
            pltpu.VMEM((2, 3, 8, 1, 128), F32),
            pltpu.VMEM((3, 8, 2, W), F32),
            dma((3, 32)), dma((3, 32)), dma((3, 2)), dma((3, 2)), dma((3,)), dma((3,)),
            dma((3, 3, 2)), dma((3, 3, 2)), dma((3, 3)), dma((3, 3)),
            dma((2, 3, 7)), dma((2, 3, 7)), dma((3, 7)), dma((3, 7)),
        ],
        compiler_params=pltpu.CompilerParams(
            collective_id=0, has_side_effects=True, vmem_limit_bytes=60 * 1024 * 1024
        ),
        name="marchenko",
    )(
        reflection,
        jnp.concatenate([starts, starts], axis=1),
        flat(focusing),
        flat(residual),
        flat(direction),
        flat(gradient),
    )
    shape = (2, ROWS, 2, K)
    return tuple(o.reshape(shape) for o in outs[:4]) + (outs[4].reshape(2, 2, K),)


def solution(mesh):
    finer = Mesh(mesh.devices.reshape(2, 2, 4, 8, 2), AXES)
    field = P(FREQ, RCV, None, None)
    return jax.shard_map(
        per_device,
        mesh=finer,
        in_specs=(P(FREQ, None, RCV, None), P(RCV, None), field, field, field, field),
        out_specs=(field, field, field, field, P(FREQ, None, None)),
        check_vma=False,
    )
```

```python
import cmath
import functools
import math

import jax
import jax.numpy as jnp
from jax import lax
from jax.experimental import pallas as pl
from jax.experimental.pallas import tpu as pltpu
from jax.sharding import Mesh
from jax.sharding import PartitionSpec as P

N = 2560
K = 192
F = 8
TS = 64
ROWS = 40
W = 2 * K
COLS = 640
TINY = 1e-06
AXES = ("freq_0", "freq_1", "rcv_0", "rcv_1", "rcv_2")
FREQ = AXES[:2]
RCV = AXES[2:]
MESH = pl.DeviceIdType.MESH
BF = jnp.bfloat16
F32 = jnp.float32


def swap(x):
    return jnp.concatenate([x[:, K:], x[:, :K]], axis=1)


def kernel(
    refl_in, starts_in, foc_in, res_in, dirn_in, grad_in,
    foc_out, res_out, dir_out, green_out, corr_out,
    refl, starts, foc_l, res_l, dirn_l, grad_l, foc, dirn,
    o_foc, o_dir, s_foc, s_res, s_dir, s_green, o_corr, i_sem, o_sem,
    gb, rbuf, rbig, rtmp, vtmp, acc, part, rs, fx, ta, tb, img, tr, ti, arb, cb,
    g_send, g_recv, x_send, x_recv, r_send, r_recv, s_send, s_recv, f_send, f_recv,
    a_send, a_recv, c_send, c_recv,
):
    xh, c, y, z, xl = (lax.axis_index(a) for a in AXES)
    q = xh * 2 + c
    pending = []

    def dev(**other):
        me = {"xh": xh, "c": c, "y": y, "z": z, "xl": xl}
        me.update(other)
        return tuple(me[n] for n in ("xh", "c", "y", "z", "xl"))

    def copy(src, dst, ss, rr, to):
        return pltpu.make_async_remote_copy(
            src_ref=src, dst_ref=dst, send_sem=ss, recv_sem=rr, device_id=to, device_id_type=MESH
        )

    def start(*args):
        d = copy(*args)
        d.start()
        pending.append(d)

    cell = []
    for i in range(1, 8):
        dx, dc, dl = i >> 2, (i >> 1) & 1, i & 1
        cell.append(((xh + dx) % 2, (c + dc) % 2, (xl + dl) % 2))
    cell_peers = [(dev(xh=a, c=b, xl=d), a * 4 + b * 2 + d) for a, b, d in cell]
    y_peers = [(dev(y=(y + i) % 4), (y + i) % 4) for i in (2, 1, 3)]
    plane = [((y + i // 8) % 4, (z + i % 8) % 8) for i in range(1, 32)]
    plane_peers = [(dev(y=a, z=b), a * 8 + b) for a, b in plane]
    x_peer = dev(xl=1 - xl)

    loads = [
        pltpu.make_async_copy(a, b, i_sem.at[i])
        for i, (a, b) in enumerate(
            [(dirn_in, dirn_l), (refl_in, refl), (foc_in, foc_l), (res_in, res_l),
             (starts_in, starts), (grad_in, grad_l)]
        )
    ]
    for d in loads:
        d.start()
    stores = []

    def store(src, dst, i):
        d = pltpu.make_async_copy(src, dst, o_sem.at[i])
        d.start()
        stores.append(d)

    def band(r):
        return pl.ds(pl.multiple_of(r * 8, 8), 8)

    def flatten(src, put):
        def one(r, _):
            for f in range(2):
                rows = band(r)
                put(f, rows, jnp.concatenate([src[f, rows, 0, :], src[f, rows, 1, :]], axis=1))
            return 0

        lax.fori_loop(0, ROWS // 8, one, 0)

    def split(dst, f, rows, v):
        dst[f, rows, 0, :] = v[:, :K]
        dst[f, rows, 1, :] = v[:, K:]

    barrier = pltpu.get_barrier_semaphore()
    everyone = [p for p, _ in cell_peers + plane_peers]
    for p in everyone:
        pl.semaphore_signal(barrier, inc=1, device_id=p, device_id_type=MESH)

    def into(dst):
        def put(f, rows, v):
            dst[f, rows, :] = v

        return put

    loads[0].wait()
    flatten(dirn_l, into(dirn))
    for f in range(2):
        gb[0, f, z, xl] = dirn[f].astype(BF)
    loads[1].wait()
    pl.semaphore_wait(barrier, len(everyone))

    order = [(0, 0), (1, 0), (0, 1), (1, 1)]

    def valid(s, way, f):
        return s < 4 or f == way

    def unit(k, f, a, zz):
        return gb.at[k, f, zz, xl if a == 0 else 1 - xl]

    def gsem(way, s, f, a):
        return ((way * 4 + s - 1) * 2 + f) * 2 + a

    seen = set()

    def wait_unit(k, way, s, f, a):
        if (k, way, s, f, a) in seen:
            return
        seen.add((k, way, s, f, a))
        zz = (z - s + 8) % 8 if way == 0 else (z + s) % 8
        u = unit(k, f, a, zz)
        i = gsem(way, s, f, a)
        copy(u, u, g_send.at[k, i], g_recv.at[k, i], x_peer).wait_recv()

    def exchange(k):
        for f in range(2):
            u = gb.at[k, f, z, xl]
            start(u, u, x_send.at[k, f], x_recv.at[k, f], x_peer)

    def ring(k, s, sides=(0, 1)):
        for f, a in order:
            if a not in sides:
                continue
            if s == 1 and a == 1:
                u = gb.at[k, f, z, 1 - xl]
                copy(u, u, x_send.at[k, f], x_recv.at[k, f], x_peer).wait_recv()
            for way in range(2):
                if not valid(s, way, f):
                    continue
                if s > 1:
                    wait_unit(k, way, s - 1, f, a)
                zz = (z - s + 9) % 8 if way == 0 else (z + s - 1) % 8
                to = dev(z=(z + 1) % 8 if way == 0 else (z + 7) % 8)
                u = unit(k, f, a, zz)
                i = gsem(way, s, f, a)
                start(u, u, g_send.at[k, i], g_recv.at[k, i], to)

    def gathered(k):
        for s in range(1, 5):
            for f, a in order:
                for way in range(2):
                    if valid(s, way, f):
                        wait_unit(k, way, s, f, a)

    lane = lax.broadcasted_iota(jnp.int32, (8, W), 1)
    sign = jnp.where(lane < K, -1.0, 1.0).astype(F32)
    sign_rows = jnp.where(
        lax.broadcasted_iota(jnp.int32, (ROWS, W), 1) < K, -1.0, 1.0
    ).astype(F32)

    def send_reflection():
        for i, (p, yy) in enumerate(y_peers):
            cols = pl.ds(pl.multiple_of(yy * COLS, 128), COLS)
            start(refl.at[:, :, :, cols], rbuf.at[y], r_send.at[i], r_recv.at[i], p)

    def assemble_reflection():
        cols = pl.ds(pl.multiple_of(y * COLS, 128), COLS)
        for f in range(2):
            for p in range(2):
                rbuf[y, f, p] = refl[f, p, :, cols]
        for i, j in enumerate((2, 3, 1)):
            src = rbuf.at[(y + j) % 4]
            copy(src, src, r_send.at[i], r_recv.at[i], x_peer).wait_recv()
        for f in range(2):

            def put(i, _, f=f):
                rows = pl.ds(pl.multiple_of(i * ROWS, 8), ROWS)
                rtmp[rows, :] = rbuf[i // 2, f, i % 2].astype(F32)
                return 0

            lax.fori_loop(0, 8, put, 0)
            rbig[f] = rtmp[...].astype(BF)

    def multiply(k, conjugate):
        for f in range(2):

            def put(i, _, f=f):
                rows = pl.ds(pl.multiple_of(i * ROWS, 8), ROWS)
                vtmp[rows, :] = gb[k, f, i // 2, i % 2].astype(F32)
                return 0

            lax.fori_loop(0, 16, put, 0)
            acc[...] = jnp.dot(rbig[f], vtmp[...].astype(BF), preferred_element_type=F32)
            for i, (p, yy) in enumerate(y_peers + [(None, y)]):
                first = acc[pl.ds(pl.multiple_of(yy * 80, 8), ROWS), :]
                second = acc[pl.ds(pl.multiple_of(yy * 80 + 40, 8), ROWS), :]
                turned = sign_rows * swap(second)
                part[k, i, f] = first - turned if conjugate else first + turned
                if p is not None:
                    start(part.at[k, i, f], rs.at[k, y, f], s_send.at[k, i, f], s_recv.at[k, i, f], p)

    def reduced(k, f):
        total = part[k, 3, f]
        for i, j in enumerate((2, 3, 1)):
            src = rs.at[k, (y + j) % 4, f]
            copy(src, src, s_send.at[k, i, f], s_recv.at[k, i, f], x_peer).wait_recv()
            total = total + rs[k, (y + j) % 4, f]
        return total

    q_c = xh * 2 + 1 - c
    q_x = (1 - xh) * 2 + c
    q_xc = (1 - xh) * 2 + 1 - c

    def share(k, f):
        u = fx.at[k, q, f]
        start(u, u, f_send.at[k, 1, f], f_recv.at[k, 1, f], dev(xh=1 - xh))
        start(u, u, f_send.at[k, 0, f], f_recv.at[k, 0, f], dev(c=1 - c))

    def relay(k):
        for f in range(2):
            u = fx.at[k, q_x, f]
            copy(u, u, f_send.at[k, 1, f], f_recv.at[k, 1, f], x_peer).wait_recv()
            start(u, u, f_send.at[k, 2, f], f_recv.at[k, 2, f], dev(c=1 - c))

    def shared(k):
        for i, qq in ((0, q_c), (2, q_xc)):
            for f in range(2):
                u = fx.at[k, qq, f]
                copy(u, u, f_send.at[k, i, f], f_recv.at[k, i, f], x_peer).wait_recv()

    def tables():
        def one(r, _):
            rows = band(r)
            s = starts[rows, :]
            s = jnp.clip(jnp.concatenate([s, s], axis=1), 0, TS)
            zr = jnp.ones((8, W), F32)
            zi = jnp.zeros((8, W), F32)
            for b in range(6):
                w = cmath.exp(2j * math.pi * (1 << b) / TS)
                on = (s & (1 << b)) != 0
                nr, ni = zr * w.real - zi * w.imag, zr * w.imag + zi * w.real
                zr, zi = jnp.where(on, nr, zr), jnp.where(on, ni, zi)
            ta[7, rows, :] = s.astype(F32) * (1.0 / TS)
            tb[7, rows, :] = jnp.zeros((8, W), F32)
            pr, pi = zr, zi
            for d in range(1, 8):
                k = 1.0 / (TS * (1.0 - cmath.exp(2j * math.pi * d / TS)))
                gr = k.real - (k.real * pr - k.imag * pi)
                gi = sign * (k.imag - (k.real * pi + k.imag * pr))
                ta[7 + d, rows, :] = gr
                ta[7 - d, rows, :] = gr
                tb[7 + d, rows, :] = gi
                tb[7 - d, rows, :] = -gi
                pr, pi = pr * zr - pi * zi, pr * zi + pi * zr
            return 0

        lax.fori_loop(0, ROWS // 8, one, 0)

    def gate_own(fields, e, rows):
        total = None
        for j, (u, v) in enumerate(fields):
            d = 7 + j - e - 2 * q
            term = ta[d, rows, :] * u + tb[d, rows, :] * v
            total = term if total is None else total + term
        return total

    def fields_of(k, rows):
        us = [fx[k, j // 2, j % 2, rows, :] for j in range(F)]
        return [(u, swap(u)) for u in us]

    def gate_residual():
        def one(r, _):
            rows = band(r)
            fields = fields_of(0, rows)
            for e in range(2):
                tr[e, rows, :] = gate_own(fields, e, rows)
            return 0

        lax.fori_loop(0, ROWS // 8, one, 0)

    def gate_image():
        def one(r, total):
            rows = band(r)
            fields = fields_of(1, rows)
            images = []
            for j in range(F):
                t = ta[7, rows, :] * fields[j][0]
                for i in range(F):
                    if i != j:
                        d = 7 + i - j
                        t = t + ta[d, rows, :] * fields[i][0] + tb[d, rows, :] * fields[i][1]
                img[j, rows, :] = t
                images.append((t, swap(t)))
                total = total + t * t
            for e in range(2):
                ti[e, rows, :] = gate_own(images, e, rows)
            return total

        return lax.fori_loop(0, ROWS // 8, one, jnp.zeros((8, W), F32))

    def squares(load):
        def one(r, total):
            for e in range(2):
                x = load(e, band(r))
                total = total + x * x
            return total

        return lax.fori_loop(0, ROWS // 8, one, jnp.zeros((8, W), F32))

    def added(x):
        x = jnp.sum(x, axis=0, keepdims=True)
        return jnp.sum(x, axis=1, keepdims=True)

    cell_slot = xh * 4 + c * 2 + xl

    def put_sum(buf, ss, rr, slot, peers, value):
        buf[slot] = value
        for i, (p, _) in enumerate(peers):
            start(buf.at[slot], buf.at[slot], ss.at[i], rr.at[i], p)

    def get_sum(buf, ss, rr, peers, back, count):
        for i, j in enumerate(back):
            u = buf.at[j]
            copy(u, u, ss.at[i], rr.at[i], x_peer).wait_recv()
        total = buf[0]
        for i in range(1, count):
            total = total + buf[i]
        return total

    cell_back = [s for _, s in cell_peers]
    plane_back = [((y + 4 - i // 8) % 4) * 8 + (z + 8 - i % 8) % 8 for i in range(1, 32)]
    phases = [(cell_slot, cell_peers, cell_back, 8), (y * 8 + z, plane_peers, plane_back, 32)]

    def sum_put(k, phase, value):
        slot, peers, _, _ = phases[phase]
        put_sum(arb.at[k, phase], a_send.at[k, phase], a_recv.at[k, phase], slot, peers, value)

    def sum_get(k, phase):
        _, peers, back, count = phases[phase]
        return get_sum(arb.at[k, phase], a_send.at[k, phase], a_recv.at[k, phase], peers, back, count)

    corr_phases = [(xl, [(x_peer, 1 - xl)], [1 - xl], 2), phases[1]]

    def corr_put(phase, value):
        slot, peers, _, _ = corr_phases[phase]
        put_sum(cb.at[phase], c_send.at[phase], c_recv.at[phase], slot, peers, value)

    def corr_get(phase):
        _, peers, back, count = corr_phases[phase]
        return get_sum(cb.at[phase], c_send.at[phase], c_recv.at[phase], peers, back, count)

    exchange(0)
    ring(0, 1, (0,))
    send_reflection()
    loads[2].wait()
    flatten(foc_l, into(foc))
    for f in range(2):
        gb[1, f, z, xl] = foc[f].astype(BF)
    ring(0, 1, (1,))
    exchange(1)
    ring(0, 2)
    loads[3].wait()
    flatten(res_l, into(fx.at[0, q]))
    for f in range(2):
        share(0, f)
    loads[4].wait()
    tables()
    ring(0, 3)
    assemble_reflection()
    ring(0, 4)
    ring(1, 1)
    loads[5].wait()

    def square(r, total):
        for f in range(2):
            g = grad_l[f, band(r)]
            total = total + g * g
        return total

    gamma_all = lax.fori_loop(0, ROWS // 8, square, jnp.zeros((8, 2, K), F32))
    gamma_own = added(jnp.sum(gamma_all, axis=0))
    relay(0)
    gathered(0)
    multiply(0, False)
    ring(1, 2)
    for f in range(2):
        fx[1, q, f] = reduced(0, f)
        share(1, f)
    ring(1, 3)
    shared(0)
    gate_residual()
    relay(1)
    shared(1)
    curvature_own = added(gate_image()) * 0.25
    half = lax.broadcasted_iota(jnp.int32, (1, 128), 1) < 64
    sum_put(0, 0, jnp.where(half, gamma_own, curvature_own))
    ring(1, 4)
    sum_put(0, 1, sum_get(0, 0))
    gathered(1)
    both = sum_get(0, 1)
    gamma, curvature = both[:, 0:1], both[:, 64:65]
    alpha = gamma / (curvature + TINY)
    for f in range(2):
        gb[2, f, z, xl] = (tr[f] - alpha * ti[f]).astype(BF)
    exchange(2)
    ring(2, 1, (0,))
    multiply(1, False)
    ring(2, 1, (1,))

    def step(r, _):
        rows = band(r)
        for f in range(2):
            v = foc[f, rows, :] + alpha * dirn[f, rows, :]
            o_foc[f, rows, :] = v
            split(s_foc, f, rows, v)
            split(s_res, f, rows, fx[0, q, f, rows, :] - alpha * img[2 * q + f, rows, :])
        return 0

    lax.fori_loop(0, ROWS // 8, step, 0)
    store(s_foc, foc_out, 0)
    store(s_res, res_out, 1)
    ring(2, 2)
    for f in range(2):
        fx[2, q, f] = reduced(1, f)
        share(2, f)
    ring(2, 3)
    ring(2, 4)
    gathered(2)
    multiply(2, True)
    relay(2)
    shared(2)

    def green(r, total):
        rows = band(r)
        fields = fields_of(2, rows)
        out = []
        for e in range(2):
            own = fx[2, q, e, rows, :]
            g = own - gate_own(fields, e, rows)
            g = g + alpha * (fx[1, q, e, rows, :] - img[2 * q + e, rows, :])
            split(s_green, e, rows, g)
            v = o_foc[e, rows, :]
            out += [total[2 * e] + g * v, total[2 * e + 1] + g * swap(v)]
        return tuple(out)

    def finish_corr():
        none = jnp.zeros((8, W), F32)
        sums = lax.fori_loop(0, ROWS // 8, green, (none, none, none, none))
        out = []
        for e in range(2):
            a = jnp.sum(sums[2 * e], axis=0, keepdims=True)
            b = jnp.sum(sums[2 * e + 1], axis=0, keepdims=True)
            out.append(jnp.where(lane[:1] < K, a + swap(a), b - swap(b)))
        return jnp.concatenate(out, axis=0)

    corr_put(0, finish_corr())
    store(s_green, green_out, 2)
    for f in range(2):
        o_dir[f] = reduced(2, f)
    sum_put(1, 0, jnp.broadcast_to(added(squares(lambda e, rows: o_dir[e, rows, :])), (1, 128)))
    corr_put(1, corr_get(0))
    sum_put(1, 1, sum_get(1, 0))
    corr = corr_get(1) * (1.0 / math.sqrt(N))
    for f in range(2):
        o_corr[f, 0:1, :] = corr[f : f + 1, :K]
        o_corr[f, 1:2, :] = corr[f : f + 1, K:]
    store(o_corr, corr_out, 3)
    new_gamma = sum_get(1, 1)[:, 0:1]
    ratio = new_gamma / (gamma + TINY)

    def last(r, _):
        rows = band(r)
        for f in range(2):
            split(s_dir, f, rows, o_dir[f, rows, :] + ratio * dirn[f, rows, :])
        return 0

    lax.fori_loop(0, ROWS // 8, last, 0)
    store(s_dir, dir_out, 4)
    for d in pending:
        d.wait_send()
    for d in stores:
        d.wait()


def emit(*refs):
    ins, outs, held, (i_sem, o_sem) = refs[:5], refs[5:10], refs[10:15], refs[15:]
    loads = [pltpu.make_async_copy(ins[i], held[i], i_sem.at[i]) for i in range(5)]
    stores = [pltpu.make_async_copy(held[i], outs[i], o_sem.at[i]) for i in range(5)]
    for d in loads:
        d.start()
    for a, b in zip(loads, stores):
        a.wait()
        b.start()
    for d in stores:
        d.wait()


def per_device(reflection, starts, focusing, residual, direction, gradient):
    field = jax.ShapeDtypeStruct((2, ROWS, 2, K), F32)
    dma = pltpu.SemaphoreType.DMA
    native = pltpu.VMEM((2, ROWS, 2, K), F32)
    flat = pltpu.VMEM((2, ROWS, W), F32)
    hbm = pl.BlockSpec(memory_space=pltpu.HBM)
    shapes = (field, field, field, field, jax.ShapeDtypeStruct((2, 2, K), F32))
    outs = pl.pallas_call(
        kernel,
        out_shape=shapes,
        in_specs=[hbm] * 6,
        out_specs=[hbm] * 5,
        scratch_shapes=[
            pltpu.VMEM((2, 2, ROWS, N), BF),
            pltpu.VMEM((ROWS, K), jnp.int32),
            native, native, native, native, flat, flat,
            flat, flat, native, native, native, native,
            pltpu.VMEM((2, 2, K), F32), dma((6,)), dma((5,)),
            pltpu.VMEM((3, 2, 8, 2, ROWS, W), BF),
            pltpu.VMEM((4, 2, 2, ROWS, COLS), BF),
            pltpu.VMEM((2, 320, COLS), BF),
            pltpu.VMEM((320, COLS), F32),
            pltpu.VMEM((COLS, W), F32),
            pltpu.VMEM((320, W), F32),
            pltpu.VMEM((3, 4, 2, ROWS, W), F32),
            pltpu.VMEM((3, 4, 2, ROWS, W), F32),
            pltpu.VMEM((3, 4, 2, ROWS, W), F32),
            pltpu.VMEM((15, ROWS, W), F32),
            pltpu.VMEM((15, ROWS, W), F32),
            pltpu.VMEM((F, ROWS, W), F32),
            pltpu.VMEM((2, ROWS, W), F32),
            pltpu.VMEM((2, ROWS, W), F32),
            pltpu.VMEM((2, 2, 32, 1, 128), F32),
            pltpu.VMEM((2, 32, 2, W), F32),
            dma((3, 32)), dma((3, 32)), dma((3, 2)), dma((3, 2)), dma((3,)), dma((3,)),
            dma((3, 3, 2)), dma((3, 3, 2)), dma((3, 3, 2)), dma((3, 3, 2)),
            dma((2, 2, 31)), dma((2, 2, 31)), dma((2, 31)), dma((2, 31)),
        ],
        compiler_params=pltpu.CompilerParams(
            collective_id=0, has_side_effects=True, vmem_limit_bytes=63 * 1024 * 1024
        ),
        name="marchenko",
    )(reflection, starts, focusing, residual, direction, gradient)
    return pl.pallas_call(
        emit,
        out_shape=shapes,
        in_specs=[hbm] * 5,
        out_specs=[hbm] * 5,
        scratch_shapes=[
            native, native, native, native, pltpu.VMEM((2, 2, K), F32), dma((5,)), dma((5,)),
        ],
        compiler_params=pltpu.CompilerParams(vmem_limit_bytes=63 * 1024 * 1024),
        name="emit",
    )(*outs)


def solution(mesh):
    finer = Mesh(mesh.devices.reshape(2, 2, 4, 8, 2), AXES)
    field = P(FREQ, RCV, None, None)
    return jax.shard_map(
        per_device,
        mesh=finer,
        in_specs=(P(FREQ, None, RCV, None), P(RCV, None), field, field, field, field),
        out_specs=(field, field, field, field, P(FREQ, None, None)),
        check_vma=False,
    )
```

```python
import cmath
import functools
import math

import jax
import jax.numpy as jnp
from jax import lax
from jax.experimental import pallas as pl
from jax.experimental.pallas import tpu as pltpu
from jax.sharding import Mesh
from jax.sharding import PartitionSpec as P

N = 2560
K = 192
F = 8
TS = 64
ROWS = 40
W = 2 * K
COLS = 640
TINY = 1e-06
AXES = ("freq_0", "freq_1", "rcv_0", "rcv_1", "rcv_2")
FREQ = AXES[:2]
RCV = AXES[2:]
MESH = pl.DeviceIdType.MESH
BF = jnp.bfloat16
F32 = jnp.float32


def swap(x):
    return jnp.concatenate([x[:, K:], x[:, :K]], axis=1)


def kernel(
    refl_in, starts_in, foc_in, res_in, dirn_in, grad_in,
    foc_out, res_out, dir_out, green_out, corr_out,
    refl, starts, foc_l, res_l, dirn_l, grad_l, foc, dirn,
    o_foc, o_dir, s_foc, s_res, s_dir, s_green, o_corr, i_sem, o_sem,
    gb, rbuf, rbig, rtmp, vtmp, acc, part, rs, fx, ta, tb, img, tr, ti, arb, cb,
    g_send, g_recv, x_send, x_recv, r_send, r_recv, s_send, s_recv, f_send, f_recv,
    a_send, a_recv, c_send, c_recv, bb, b_send, b_recv,
):
    xh, c, y, z, xl = (lax.axis_index(a) for a in AXES)
    q = xh * 2 + c

    def dev(**other):
        me = {"xh": xh, "c": c, "y": y, "z": z, "xl": xl}
        me.update(other)
        return tuple(me[n] for n in ("xh", "c", "y", "z", "xl"))

    def copy(src, dst, ss, rr, to):
        return pltpu.make_async_remote_copy(
            src_ref=src, dst_ref=dst, send_sem=ss, recv_sem=rr, device_id=to, device_id_type=MESH
        )

    def start(*args):
        copy(*args).start()

    def sent(ref, sem):
        copy(ref, ref, sem, sem, x_peer).wait_send()

    def came(ref, sem):
        copy(ref, ref, sem, sem, x_peer).wait_recv()

    cell = []
    for i in range(1, 8):
        dx, dc, dl = i >> 2, (i >> 1) & 1, i & 1
        cell.append(((xh + dx) % 2, (c + dc) % 2, (xl + dl) % 2))
    cell_peers = [(dev(xh=a, c=b, xl=d), a * 4 + b * 2 + d) for a, b, d in cell]
    y_peers = [(dev(y=(y + i) % 4), (y + i) % 4) for i in (2, 1, 3)]
    plane = [((y + i // 8) % 4, (z + i % 8) % 8) for i in range(1, 32)]
    plane_peers = [(dev(y=a, z=b), a * 8 + b) for a, b in plane]
    x_peer = dev(xl=1 - xl)
    block = [((xl + i // 32) % 2, (y + i // 8 % 4) % 4, (z + i % 8) % 8) for i in range(1, 64)]
    block_peers = [(dev(xl=a, y=b, z=d), (b * 8 + d) * 2 + a) for a, b, d in block]

    loads = [
        pltpu.make_async_copy(a, b, i_sem.at[i])
        for i, (a, b) in enumerate(
            [(dirn_in, dirn_l), (refl_in, refl), (foc_in, foc_l), (res_in, res_l),
             (starts_in, starts), (grad_in, grad_l)]
        )
    ]
    for d in loads:
        d.start()
    stores = []

    def store(src, dst, i):
        d = pltpu.make_async_copy(src, dst, o_sem.at[i])
        d.start()
        stores.append(d)

    def band(r):
        return pl.ds(pl.multiple_of(r * 8, 8), 8)

    def flatten(src, put):
        def one(r, _):
            for f in range(2):
                rows = band(r)
                put(f, rows, jnp.concatenate([src[f, rows, 0, :], src[f, rows, 1, :]], axis=1))
            return 0

        lax.fori_loop(0, ROWS // 8, one, 0)

    def split(dst, f, rows, v):
        dst[f, rows, 0, :] = v[:, :K]
        dst[f, rows, 1, :] = v[:, K:]

    barrier = pltpu.get_barrier_semaphore()
    near = [dev(z=(z + i) % 8, xl=a) for i in (1, 7) for a in (xl, 1 - xl)]
    everyone = [p for p, _ in cell_peers + y_peers] + near
    for p in everyone:
        pl.semaphore_signal(barrier, inc=1, device_id=p, device_id_type=MESH)

    def into(dst):
        def put(f, rows, v):
            dst[f, rows, :] = v

        return put

    loads[0].wait()
    flatten(dirn_l, into(dirn))
    for f in range(2):
        gb[0, f, z, xl] = dirn[f].astype(BF)
    loads[1].wait()
    pl.semaphore_wait(barrier, len(everyone))

    order = [(0, 0), (1, 0), (0, 1), (1, 1)]

    def valid(s, way, f):
        return s < 4 or f == way

    def unit(k, f, a, zz):
        return gb.at[k, f, zz, xl if a == 0 else 1 - xl]

    def gsem(way, s, f, a):
        return (way * 3 + s - 1) * 4 + f * 2 + a if s < 4 else 24 + way * 2 + a

    seen = set()

    def wait_unit(k, way, s, f, a):
        if (k, way, s, f, a) in seen:
            return
        seen.add((k, way, s, f, a))
        zz = (z - s + 8) % 8 if way == 0 else (z + s) % 8
        u = unit(k, f, a, zz)
        i = gsem(way, s, f, a)
        fresh.append((k, f, zz, xl if a == 0 else 1 - xl))
        came(u, g_recv.at[k, i])

    def exchange(k):
        for f in range(2):
            u = gb.at[k, f, z, xl]
            start(u, u, x_send.at[k], x_recv.at[k], x_peer)

    def ring(k, s, sides=(0, 1)):
        for f, a in order:
            if a not in sides:
                continue
            for way in range(2):
                if not valid(s, way, f):
                    continue
                if s > 1:
                    wait_unit(k, way, s - 1, f, a)
                zz = (z - s + 9) % 8 if way == 0 else (z + s - 1) % 8
                far = (z + 1) % 8 if way == 0 else (z + 7) % 8
                i = gsem(way, s, f, a)
                if s == 1:
                    u = gb.at[k, f, z, xl]
                    to = dev(z=far) if a == 0 else dev(z=far, xl=1 - xl)
                else:
                    u = unit(k, f, a, zz)
                    to = dev(z=far)
                start(u, u, g_send.at[k], g_recv.at[k, i], to)

    def lay(k, f, zz, xx):
        i = zz * 2 + xx
        rows = pl.ds(pl.multiple_of(i * ROWS, 8), ROWS)
        vtmp[f, rows, :] = gb[k, f, zz, xx].astype(F32)

    fresh = []

    def drain(k):
        for kk, f, zz, xx in [v for v in fresh if v[0] == k]:
            lay(k, f, zz, xx)
        fresh[:] = [v for v in fresh if v[0] != k]

    def gathered(k):
        came(gb.at[k, :, z, 1 - xl], x_recv.at[k])
        for f in range(2):
            fresh.append((k, f, z, 1 - xl))
            fresh.append((k, f, z, xl))
        for s in range(1, 5):
            if s == 4:
                drain(k) if k != 1 else None
            for f, a in order:
                for way in range(2):
                    if valid(s, way, f):
                        wait_unit(k, way, s, f, a)

    lane = lax.broadcasted_iota(jnp.int32, (8, W), 1)
    sign = jnp.where(lane < K, -1.0, 1.0).astype(F32)
    sign_rows = jnp.where(
        lax.broadcasted_iota(jnp.int32, (ROWS, W), 1) < K, -1.0, 1.0
    ).astype(F32)

    def send_reflection():
        for p, yy in y_peers:
            cols = pl.ds(pl.multiple_of(yy * COLS, 128), COLS)
            start(refl.at[:, :, :, cols], rbuf.at[y], r_send, r_recv, p)

    def assemble_reflection():
        cols = pl.ds(pl.multiple_of(y * COLS, 128), COLS)
        for f in range(2):
            for p in range(2):
                rbuf[y, f, p] = refl[f, p, :, cols]
        came(rbuf.at[0:3], r_recv)
        for f in range(2):

            def put(i, _, f=f):
                rows = pl.ds(pl.multiple_of(i * ROWS, 8), ROWS)
                rtmp[rows, :] = rbuf[i // 2, f, i % 2].astype(F32)
                return 0

            lax.fori_loop(0, 8, put, 0)
            rbig[f] = rtmp[...].astype(BF)

    def multiply(k, conjugate):
        drain(k)
        for f in range(2):
            acc[...] = jnp.dot(rbig[f], vtmp[f].astype(BF), preferred_element_type=F32)
            for i, (p, yy) in enumerate(y_peers + [(None, y)]):
                first = acc[pl.ds(pl.multiple_of(yy * 80, 8), ROWS), :]
                second = acc[pl.ds(pl.multiple_of(yy * 80 + 40, 8), ROWS), :]
                turned = sign_rows * swap(second)
                part[k, i, f] = first - turned if conjugate else first + turned
                if p is not None:
                    start(part.at[k, i, f], rs.at[k, y, f], s_send.at[k], s_recv.at[k, f], p)

    def reduced(k, f):
        total = part[k, 3, f]
        came(rs.at[k, 0:3, f], s_recv.at[k, f])
        for j in (2, 3, 1):
            total = total + rs[k, (y + j) % 4, f]
        return total

    q_c = xh * 2 + 1 - c
    q_x = (1 - xh) * 2 + c
    q_xc = (1 - xh) * 2 + 1 - c

    def share(k, f):
        u = fx.at[k, q, f]
        start(u, u, f_send.at[k], f_recv.at[k, f], dev(xh=1 - xh))
        start(u, u, f_send.at[k], f_recv.at[k, 2], dev(c=1 - c))

    def relay(k):
        for f in range(2):
            u = fx.at[k, q_x, f]
            came(u, f_recv.at[k, f])
            start(u, u, f_send.at[k], f_recv.at[k, 2], dev(c=1 - c))

    def shared(k):
        came(fx.at[k, 0:2], f_recv.at[k, 2])

    def tables():
        def one(r, _):
            rows = band(r)
            s = starts[rows, :]
            s = jnp.clip(jnp.concatenate([s, s], axis=1), 0, TS)
            zr = jnp.ones((8, W), F32)
            zi = jnp.zeros((8, W), F32)
            for b in range(6):
                w = cmath.exp(2j * math.pi * (1 << b) / TS)
                on = (s & (1 << b)) != 0
                nr, ni = zr * w.real - zi * w.imag, zr * w.imag + zi * w.real
                zr, zi = jnp.where(on, nr, zr), jnp.where(on, ni, zi)
            ta[7, rows, :] = s.astype(F32) * (1.0 / TS)
            tb[7, rows, :] = jnp.zeros((8, W), F32)
            pr, pi = zr, zi
            for d in range(1, 8):
                k = 1.0 / (TS * (1.0 - cmath.exp(2j * math.pi * d / TS)))
                gr = k.real - (k.real * pr - k.imag * pi)
                gi = sign * (k.imag - (k.real * pi + k.imag * pr))
                ta[7 + d, rows, :] = gr
                ta[7 - d, rows, :] = gr
                tb[7 + d, rows, :] = gi
                tb[7 - d, rows, :] = -gi
                pr, pi = pr * zr - pi * zi, pr * zi + pi * zr
            return 0

        lax.fori_loop(0, ROWS // 8, one, 0)

    def gate_own(fields, e, rows):
        total = None
        for j, (u, v) in enumerate(fields):
            d = 7 + j - e - 2 * q
            term = ta[d, rows, :] * u + tb[d, rows, :] * v
            total = term if total is None else total + term
        return total

    def fields_of(k, rows):
        us = [fx[k, j // 2, j % 2, rows, :] for j in range(F)]
        return [(u, swap(u)) for u in us]

    def gate_residual():
        def one(r, _):
            rows = band(r)
            fields = fields_of(0, rows)
            for e in range(2):
                tr[e, rows, :] = gate_own(fields, e, rows)
            return 0

        lax.fori_loop(0, ROWS // 8, one, 0)

    def gate_image():
        def one(r, total):
            rows = band(r)
            fields = fields_of(1, rows)
            images = []
            for j in range(F):
                t = ta[7, rows, :] * fields[j][0]
                for i in range(F):
                    if i != j:
                        d = 7 + i - j
                        t = t + ta[d, rows, :] * fields[i][0] + tb[d, rows, :] * fields[i][1]
                img[j, rows, :] = t
                images.append((t, swap(t)))
                total = total + t * t
            for e in range(2):
                ti[e, rows, :] = gate_own(images, e, rows)
            return total

        return lax.fori_loop(0, ROWS // 8, one, jnp.zeros((8, W), F32))

    def squares(load):
        def one(r, total):
            for e in range(2):
                x = load(e, band(r))
                total = total + x * x
            return total

        return lax.fori_loop(0, ROWS // 8, one, jnp.zeros((8, W), F32))

    def added(x):
        x = jnp.sum(x, axis=0, keepdims=True)
        return jnp.sum(x, axis=1, keepdims=True)

    cell_slot = xh * 4 + c * 2 + xl

    def put_sum(buf, ss, rr, slot, peers, value):
        buf[slot] = value
        for p, _ in peers:
            start(buf.at[slot], buf.at[slot], ss, rr, p)

    def get_sum(buf, ss, rr, count):
        came(buf.at[0 : count - 1], rr)
        sent(buf.at[0 : count - 1], ss)
        total = buf[0]
        for i in range(1, count):
            total = total + buf[i]
        return total

    phases = [(cell_slot, cell_peers, 8), (y * 8 + z, plane_peers, 32)]

    def sum_put(k, phase, value):
        slot, peers, _ = phases[phase]
        put_sum(arb.at[k, phase], a_send.at[k, phase], a_recv.at[k, phase], slot, peers, value)

    def sum_get(k, phase):
        return get_sum(arb.at[k, phase], a_send.at[k, phase], a_recv.at[k, phase], phases[phase][2])

    corr_phases = [(xl, [(x_peer, 1 - xl)], 2), phases[1]]

    def corr_put(phase, value):
        slot, peers, _ = corr_phases[phase]
        put_sum(cb.at[phase], c_send.at[phase], c_recv.at[phase], slot, peers, value)

    def corr_get(phase):
        return get_sum(cb.at[phase], c_send.at[phase], c_recv.at[phase], corr_phases[phase][2])

    ring(0, 1)
    exchange(0)
    send_reflection()
    loads[2].wait()
    flatten(foc_l, into(foc))
    for f in range(2):
        gb[1, f, z, xl] = foc[f].astype(BF)
    ring(0, 2)
    loads[3].wait()
    flatten(res_l, into(fx.at[0, q]))
    for f in range(2):
        share(0, f)
    loads[4].wait()
    ring(0, 3)
    drain(0)
    tables()
    ring(0, 4)
    ring(1, 1)
    exchange(1)
    drain(0)
    assemble_reflection()
    loads[5].wait()

    def square(r, total):
        for f in range(2):
            g = grad_l[f, band(r)]
            total = total + g * g
        return total

    gamma_all = lax.fori_loop(0, ROWS // 8, square, jnp.zeros((8, 2, K), F32))
    gamma_own = added(jnp.sum(gamma_all, axis=0))
    sum_put(0, 0, jnp.broadcast_to(gamma_own, (1, 128)))
    relay(0)
    gathered(0)
    multiply(0, False)
    ring(1, 2)
    for f in range(2):
        fx[1, q, f] = reduced(0, f)
        share(1, f)
    sum_put(0, 1, sum_get(0, 0))
    ring(1, 3)
    shared(0)
    gate_residual()
    relay(1)
    shared(1)
    curvature_own = added(gate_image())
    block_slot = (y * 8 + z) * 2 + xl
    put_sum(bb, b_send, b_recv, block_slot, block_peers, jnp.broadcast_to(curvature_own, (1, 128)))
    ring(1, 4)
    gamma = sum_get(0, 1)[:, 0:1]
    gathered(1)
    curvature = get_sum(bb, b_send, b_recv, 64)[:, 0:1]
    alpha = gamma / (curvature + TINY)
    for f in range(2):
        gb[2, f, z, xl] = (tr[f] - alpha * ti[f]).astype(BF)
    ring(2, 1)
    exchange(2)
    multiply(1, False)

    def step(r, _):
        rows = band(r)
        for f in range(2):
            v = foc[f, rows, :] + alpha * dirn[f, rows, :]
            o_foc[f, rows, :] = v
            split(s_foc, f, rows, v)
            split(s_res, f, rows, fx[0, q, f, rows, :] - alpha * img[2 * q + f, rows, :])
        return 0

    ring(2, 2)
    lax.fori_loop(0, ROWS // 8, step, 0)
    store(s_foc, foc_out, 0)
    store(s_res, res_out, 1)
    drain(2)
    for f in range(2):
        fx[2, q, f] = reduced(1, f)
        share(2, f)
    ring(2, 3)
    drain(2)
    ring(2, 4)
    drain(2)
    gathered(2)
    multiply(2, True)
    relay(2)
    shared(2)

    def green(r, total):
        rows = band(r)
        fields = fields_of(2, rows)
        out = []
        for e in range(2):
            own = fx[2, q, e, rows, :]
            g = own - gate_own(fields, e, rows)
            g = g + alpha * (fx[1, q, e, rows, :] - img[2 * q + e, rows, :])
            split(s_green, e, rows, g)
            v = o_foc[e, rows, :]
            out += [total[2 * e] + g * v, total[2 * e + 1] + g * swap(v)]
        return tuple(out)

    def finish_corr():
        none = jnp.zeros((8, W), F32)
        sums = lax.fori_loop(0, ROWS // 8, green, (none, none, none, none))
        out = []
        for e in range(2):
            a = jnp.sum(sums[2 * e], axis=0, keepdims=True)
            b = jnp.sum(sums[2 * e + 1], axis=0, keepdims=True)
            out.append(jnp.where(lane[:1] < K, a + swap(a), b - swap(b)))
        return jnp.concatenate(out, axis=0)

    corr_put(0, finish_corr())
    store(s_green, green_out, 2)
    for f in range(2):
        o_dir[f] = reduced(2, f)
    sum_put(1, 0, jnp.broadcast_to(added(squares(lambda e, rows: o_dir[e, rows, :])), (1, 128)))
    corr_put(1, corr_get(0))
    sum_put(1, 1, sum_get(1, 0))
    corr = corr_get(1) * (1.0 / math.sqrt(N))
    for f in range(2):
        o_corr[f, 0:1, :] = corr[f : f + 1, :K]
        o_corr[f, 1:2, :] = corr[f : f + 1, K:]
    store(o_corr, corr_out, 3)
    new_gamma = sum_get(1, 1)[:, 0:1]
    ratio = new_gamma / (gamma + TINY)

    def last(r, _):
        rows = band(r)
        for f in range(2):
            split(s_dir, f, rows, o_dir[f, rows, :] + ratio * dirn[f, rows, :])
        return 0

    lax.fori_loop(0, ROWS // 8, last, 0)
    store(s_dir, dir_out, 4)
    sent(rbuf.at[0:3], r_send)
    for k in range(3):
        sent(gb.at[k, :, 0:7], g_send.at[k])
        sent(gb.at[k, :, 0, 0], x_send.at[k])
        sent(part.at[k, 0:3], s_send.at[k])
        sent(fx.at[k, 0:3], f_send.at[k])
    for d in stores:
        d.wait()


def emit(*refs):
    ins, outs, held, (i_sem, o_sem) = refs[:5], refs[5:10], refs[10:15], refs[15:]
    loads = [pltpu.make_async_copy(ins[i], held[i], i_sem.at[i]) for i in range(5)]
    stores = [pltpu.make_async_copy(held[i], outs[i], o_sem.at[i]) for i in range(5)]
    for d in loads:
        d.start()
    for a, b in zip(loads, stores):
        a.wait()
        b.start()
    for d in stores:
        d.wait()


def per_device(reflection, starts, focusing, residual, direction, gradient):
    field = jax.ShapeDtypeStruct((2, ROWS, 2, K), F32)
    dma = pltpu.SemaphoreType.DMA
    native = pltpu.VMEM((2, ROWS, 2, K), F32)
    flat = pltpu.VMEM((2, ROWS, W), F32)
    hbm = pl.BlockSpec(memory_space=pltpu.HBM)
    shapes = (field, field, field, field, jax.ShapeDtypeStruct((2, 2, K), F32))
    outs = pl.pallas_call(
        kernel,
        out_shape=shapes,
        in_specs=[hbm] * 6,
        out_specs=[hbm] * 5,
        scratch_shapes=[
            pltpu.VMEM((2, 2, ROWS, N), BF),
            pltpu.VMEM((ROWS, K), jnp.int32),
            native, native, native, native, flat, flat,
            flat, flat, native, native, native, native,
            pltpu.VMEM((2, 2, K), F32), dma((6,)), dma((5,)),
            pltpu.VMEM((3, 2, 8, 2, ROWS, W), BF),
            pltpu.VMEM((4, 2, 2, ROWS, COLS), BF),
            pltpu.VMEM((2, 320, COLS), BF),
            pltpu.VMEM((320, COLS), F32),
            pltpu.VMEM((2, COLS, W), F32),
            pltpu.VMEM((320, W), F32),
            pltpu.VMEM((3, 4, 2, ROWS, W), F32),
            pltpu.VMEM((3, 4, 2, ROWS, W), F32),
            pltpu.VMEM((3, 4, 2, ROWS, W), F32),
            pltpu.VMEM((15, ROWS, W), F32),
            pltpu.VMEM((15, ROWS, W), F32),
            pltpu.VMEM((F, ROWS, W), F32),
            pltpu.VMEM((2, ROWS, W), F32),
            pltpu.VMEM((2, ROWS, W), F32),
            pltpu.VMEM((2, 2, 32, 1, 128), F32),
            pltpu.VMEM((2, 32, 2, W), F32),
            dma((3,)), dma((3, 28)), dma((3,)), dma((3,)), dma, dma,
            dma((3,)), dma((3, 2)), dma((3,)), dma((3, 3)),
            dma((2, 2)), dma((2, 2)), dma((2,)), dma((2,)),
            pltpu.VMEM((64, 1, 128), F32), dma, dma,
        ],
        compiler_params=pltpu.CompilerParams(
            collective_id=0, has_side_effects=True, vmem_limit_bytes=63 * 1024 * 1024
        ),
        name="marchenko",
    )(reflection, starts, focusing, residual, direction, gradient)
    return pl.pallas_call(
        emit,
        out_shape=shapes,
        in_specs=[hbm] * 5,
        out_specs=[hbm] * 5,
        scratch_shapes=[
            native, native, native, native, pltpu.VMEM((2, 2, K), F32), dma((5,)), dma((5,)),
        ],
        compiler_params=pltpu.CompilerParams(vmem_limit_bytes=63 * 1024 * 1024),
        name="emit",
    )(*outs)


def solution(mesh):
    finer = Mesh(mesh.devices.reshape(2, 2, 4, 8, 2), AXES)
    field = P(FREQ, RCV, None, None)
    return jax.shard_map(
        per_device,
        mesh=finer,
        in_specs=(P(FREQ, None, RCV, None), P(RCV, None), field, field, field, field),
        out_specs=(field, field, field, field, P(FREQ, None, None)),
        check_vma=False,
    )
```

```python
import cmath
import functools
import math

import jax
import jax.numpy as jnp
from jax import lax
from jax.experimental import pallas as pl
from jax.experimental.pallas import tpu as pltpu
from jax.sharding import Mesh
from jax.sharding import PartitionSpec as P

N = 2560
K = 192
F = 8
TS = 64
ROWS = 40
W = 2 * K
COLS = 640
TINY = 1e-06
AXES = ("freq_0", "freq_1", "rcv_0", "rcv_1", "rcv_2")
FREQ = AXES[:2]
RCV = AXES[2:]
MESH = pl.DeviceIdType.MESH
BF = jnp.bfloat16
F32 = jnp.float32


def swap(x):
    return jnp.concatenate([x[:, K:], x[:, :K]], axis=1)


def kernel(
    refl_in, starts_in, foc_in, res_in, dirn_in, grad_in,
    foc_out, res_out, dir_out, green_out, corr_out,
    refl, starts, foc_l, res_l, dirn_l, grad_l, foc, dirn,
    o_foc, o_dir, s_foc, s_res, s_dir, s_green, o_corr, i_sem, o_sem,
    gb, rbuf, rbig, rtmp, vtmp, acc, part, rs, fx, ta, tb, img, tr, ti, arb, cb,
    g_send, g_recv, x_send, x_recv, r_send, r_recv, s_send, s_recv, f_send, f_recv,
    a_send, a_recv, c_send, c_recv, bb, b_send, b_recv,
):
    xh, c, y, z, xl = (lax.axis_index(a) for a in AXES)
    q = xh * 2 + c

    def dev(**other):
        me = {"xh": xh, "c": c, "y": y, "z": z, "xl": xl}
        me.update(other)
        return tuple(me[n] for n in ("xh", "c", "y", "z", "xl"))

    def copy(src, dst, ss, rr, to):
        return pltpu.make_async_remote_copy(
            src_ref=src, dst_ref=dst, send_sem=ss, recv_sem=rr, device_id=to, device_id_type=MESH
        )

    def start(*args):
        copy(*args).start()

    def sent(ref, sem):
        copy(ref, ref, sem, sem, x_peer).wait_send()

    def came(ref, sem):
        copy(ref, ref, sem, sem, x_peer).wait_recv()

    cell = []
    for i in range(1, 8):
        dx, dc, dl = i >> 2, (i >> 1) & 1, i & 1
        cell.append(((xh + dx) % 2, (c + dc) % 2, (xl + dl) % 2))
    cell_peers = [(dev(xh=a, c=b, xl=d), a * 4 + b * 2 + d) for a, b, d in cell]
    y_peers = [(dev(y=(y + i) % 4), (y + i) % 4) for i in (2, 1, 3)]
    plane = [((y + i // 8) % 4, (z + i % 8) % 8) for i in range(1, 32)]
    plane_peers = [(dev(y=a, z=b), a * 8 + b) for a, b in plane]
    x_peer = dev(xl=1 - xl)
    block = [((xl + i // 32) % 2, (y + i // 8 % 4) % 4, (z + i % 8) % 8) for i in range(1, 64)]
    block_peers = [(dev(xl=a, y=b, z=d), (b * 8 + d) * 2 + a) for a, b, d in block]

    barrier = pltpu.get_barrier_semaphore()
    near = [dev(z=(z + i) % 8, xl=a) for i in (1, 7) for a in (xl, 1 - xl)]
    everyone = [p for p, _ in cell_peers + y_peers] + near
    for p in everyone:
        pl.semaphore_signal(barrier, inc=1, device_id=p, device_id_type=MESH)

    loads = [
        pltpu.make_async_copy(a, b, i_sem.at[i])
        for i, (a, b) in enumerate(
            [(dirn_in, dirn_l), (refl_in, refl), (foc_in, foc_l), (res_in, res_l),
             (starts_in, starts), (grad_in, grad_l)]
        )
    ]
    for d in loads:
        d.start()
    stores = []

    def store(src, dst, i):
        d = pltpu.make_async_copy(src, dst, o_sem.at[i])
        d.start()
        stores.append(d)

    def band(r):
        return pl.ds(pl.multiple_of(r * 8, 8), 8)

    def flatten(src, put):
        def one(r, _):
            for f in range(2):
                rows = band(r)
                put(f, rows, jnp.concatenate([src[f, rows, 0, :], src[f, rows, 1, :]], axis=1))
            return 0

        lax.fori_loop(0, ROWS // 8, one, 0)

    def split(dst, f, rows, v):
        dst[f, rows, 0, :] = v[:, :K]
        dst[f, rows, 1, :] = v[:, K:]

    def into(dst):
        def put(f, rows, v):
            dst[f, rows, :] = v

        return put

    loads[0].wait()
    flatten(dirn_l, into(dirn))
    for f in range(2):
        gb[0, f, z, xl] = dirn[f].astype(BF)
    loads[1].wait()
    pl.semaphore_wait(barrier, len(everyone))

    order = [(0, 0), (1, 0), (0, 1), (1, 1)]

    def valid(s, way, f):
        return s < 4 or f == way

    def unit(k, f, a, zz):
        return gb.at[k, f, zz, xl if a == 0 else 1 - xl]

    def gsem(way, s, f, a):
        return (way * 3 + s - 1) * 4 + f * 2 + a if s < 4 else 24 + way * 2 + a

    seen = set()

    def wait_unit(k, way, s, f, a):
        if (k, way, s, f, a) in seen:
            return
        seen.add((k, way, s, f, a))
        zz = (z - s + 8) % 8 if way == 0 else (z + s) % 8
        u = unit(k, f, a, zz)
        i = gsem(way, s, f, a)
        fresh.append((k, f, zz, xl if a == 0 else 1 - xl))
        came(u, g_recv.at[k, i])

    def exchange(k):
        for f in range(2):
            u = gb.at[k, f, z, xl]
            start(u, u, x_send.at[k], x_recv.at[k], x_peer)

    def ring(k, s, sides=(0, 1)):
        for f, a in order:
            if a not in sides:
                continue
            for way in range(2):
                if not valid(s, way, f):
                    continue
                if s > 1:
                    wait_unit(k, way, s - 1, f, a)
                zz = (z - s + 9) % 8 if way == 0 else (z + s - 1) % 8
                far = (z + 1) % 8 if way == 0 else (z + 7) % 8
                i = gsem(way, s, f, a)
                if s == 1:
                    u = gb.at[k, f, z, xl]
                    to = dev(z=far) if a == 0 else dev(z=far, xl=1 - xl)
                else:
                    u = unit(k, f, a, zz)
                    to = dev(z=far)
                start(u, u, g_send.at[k], g_recv.at[k, i], to)

    def lay(k, f, zz, xx):
        i = zz * 2 + xx
        rows = pl.ds(pl.multiple_of(i * ROWS, 8), ROWS)
        vtmp[f, rows, :] = gb[k, f, zz, xx].astype(F32)

    fresh = []

    def drain(k):
        for kk, f, zz, xx in [v for v in fresh if v[0] == k]:
            lay(k, f, zz, xx)
        fresh[:] = [v for v in fresh if v[0] != k]

    def gathered(k):
        came(gb.at[k, :, z, 1 - xl], x_recv.at[k])
        for f in range(2):
            fresh.append((k, f, z, 1 - xl))
            fresh.append((k, f, z, xl))
        for s in range(1, 5):
            if s == 4:
                drain(k) if k != 1 else None
            for f, a in order:
                for way in range(2):
                    if valid(s, way, f):
                        wait_unit(k, way, s, f, a)

    lane = lax.broadcasted_iota(jnp.int32, (8, W), 1)
    sign = jnp.where(lane < K, -1.0, 1.0).astype(F32)
    sign_rows = jnp.where(
        lax.broadcasted_iota(jnp.int32, (ROWS, W), 1) < K, -1.0, 1.0
    ).astype(F32)

    def send_reflection():
        for p, yy in y_peers:
            cols = pl.ds(pl.multiple_of(yy * COLS, 128), COLS)
            start(refl.at[:, :, :, cols], rbuf.at[y], r_send, r_recv, p)

    def assemble_reflection():
        cols = pl.ds(pl.multiple_of(y * COLS, 128), COLS)
        for f in range(2):
            for p in range(2):
                rbuf[y, f, p] = refl[f, p, :, cols]
        came(rbuf.at[0:3], r_recv)
        for f in range(2):

            def put(i, _, f=f):
                rows = pl.ds(pl.multiple_of(i * ROWS, 8), ROWS)
                rtmp[rows, :] = rbuf[i // 2, f, i % 2].astype(F32)
                return 0

            lax.fori_loop(0, 8, put, 0)
            rbig[f] = rtmp[...].astype(BF)

    def multiply(k, conjugate):
        drain(k)
        for f in range(2):
            acc[...] = jnp.dot(rbig[f], vtmp[f].astype(BF), preferred_element_type=F32)
            for i, (p, yy) in enumerate(y_peers + [(None, y)]):
                first = acc[pl.ds(pl.multiple_of(yy * 80, 8), ROWS), :]
                second = acc[pl.ds(pl.multiple_of(yy * 80 + 40, 8), ROWS), :]
                turned = sign_rows * swap(second)
                part[k, i, f] = first - turned if conjugate else first + turned
                if p is not None:
                    start(part.at[k, i, f], rs.at[k, y, f], s_send.at[k], s_recv.at[k, f], p)

    def reduced(k, f):
        total = part[k, 3, f]
        came(rs.at[k, 0:3, f], s_recv.at[k, f])
        for j in (2, 3, 1):
            total = total + rs[k, (y + j) % 4, f]
        return total

    q_c = xh * 2 + 1 - c
    q_x = (1 - xh) * 2 + c
    q_xc = (1 - xh) * 2 + 1 - c

    def share(k, f):
        u = fx.at[k, q, f]
        start(u, u, f_send.at[k], f_recv.at[k, f], dev(xh=1 - xh))
        start(u, u, f_send.at[k], f_recv.at[k, 2], dev(c=1 - c))

    def relay(k):
        for f in range(2):
            u = fx.at[k, q_x, f]
            came(u, f_recv.at[k, f])
            start(u, u, f_send.at[k], f_recv.at[k, 2], dev(c=1 - c))

    def shared(k):
        came(fx.at[k, 0:2], f_recv.at[k, 2])

    def tables():
        def one(r, _):
            rows = band(r)
            s = starts[rows, :]
            s = jnp.clip(jnp.concatenate([s, s], axis=1), 0, TS)
            zr = jnp.ones((8, W), F32)
            zi = jnp.zeros((8, W), F32)
            for b in range(6):
                w = cmath.exp(2j * math.pi * (1 << b) / TS)
                on = (s & (1 << b)) != 0
                nr, ni = zr * w.real - zi * w.imag, zr * w.imag + zi * w.real
                zr, zi = jnp.where(on, nr, zr), jnp.where(on, ni, zi)
            ta[7, rows, :] = s.astype(F32) * (1.0 / TS)
            tb[7, rows, :] = jnp.zeros((8, W), F32)
            pr, pi = zr, zi
            for d in range(1, 8):
                k = 1.0 / (TS * (1.0 - cmath.exp(2j * math.pi * d / TS)))
                gr = k.real - (k.real * pr - k.imag * pi)
                gi = sign * (k.imag - (k.real * pi + k.imag * pr))
                ta[7 + d, rows, :] = gr
                ta[7 - d, rows, :] = gr
                tb[7 + d, rows, :] = gi
                tb[7 - d, rows, :] = -gi
                pr, pi = pr * zr - pi * zi, pr * zi + pi * zr
            return 0

        lax.fori_loop(0, ROWS // 8, one, 0)

    def gate_own(fields, e, rows):
        total = None
        for j, (u, v) in enumerate(fields):
            d = 7 + j - e - 2 * q
            term = ta[d, rows, :] * u + tb[d, rows, :] * v
            total = term if total is None else total + term
        return total

    def fields_of(k, rows):
        us = [fx[k, j // 2, j % 2, rows, :] for j in range(F)]
        return [(u, swap(u)) for u in us]

    def gate_residual():
        def one(r, _):
            rows = band(r)
            fields = fields_of(0, rows)
            for e in range(2):
                tr[e, rows, :] = gate_own(fields, e, rows)
            return 0

        lax.fori_loop(0, ROWS // 8, one, 0)

    def gate_image():
        def one(r, total):
            rows = band(r)
            fields = fields_of(1, rows)
            for j in range(F):
                t = ta[7, rows, :] * fields[j][0]
                for i in range(F):
                    if i != j:
                        d = 7 + i - j
                        t = t + ta[d, rows, :] * fields[i][0] + tb[d, rows, :] * fields[i][1]
                img[j, rows, :] = t
                total = total + t * t
            return total

        return lax.fori_loop(0, ROWS // 8, one, jnp.zeros((8, W), F32))

    def gate_again():
        def one(r, _):
            rows = band(r)
            images = [img[j, rows, :] for j in range(F)]
            images = [(u, swap(u)) for u in images]
            for e in range(2):
                ti[e, rows, :] = gate_own(images, e, rows)
            return 0

        lax.fori_loop(0, ROWS // 8, one, 0)

    def squares(load):
        def one(r, total):
            for e in range(2):
                x = load(e, band(r))
                total = total + x * x
            return total

        return lax.fori_loop(0, ROWS // 8, one, jnp.zeros((8, W), F32))

    def added(x):
        x = jnp.sum(x, axis=0, keepdims=True)
        return jnp.sum(x, axis=1, keepdims=True)

    cell_slot = xh * 4 + c * 2 + xl

    def put_sum(buf, ss, rr, slot, peers, value):
        buf[slot] = value
        for p, _ in peers:
            start(buf.at[slot], buf.at[slot], ss, rr, p)

    def get_sum(buf, ss, rr, count):
        came(buf.at[0 : count - 1], rr)
        sent(buf.at[0 : count - 1], ss)
        total = buf[0]
        for i in range(1, count):
            total = total + buf[i]
        return total

    phases = [(cell_slot, cell_peers, 8), (y * 8 + z, plane_peers, 32)]

    def sum_put(k, phase, value):
        slot, peers, _ = phases[phase]
        put_sum(arb.at[k, phase], a_send.at[k, phase], a_recv.at[k, phase], slot, peers, value)

    def sum_get(k, phase):
        return get_sum(arb.at[k, phase], a_send.at[k, phase], a_recv.at[k, phase], phases[phase][2])

    corr_phases = [(xl, [(x_peer, 1 - xl)], 2), phases[1]]

    def corr_put(phase, value):
        slot, peers, _ = corr_phases[phase]
        put_sum(cb.at[phase], c_send.at[phase], c_recv.at[phase], slot, peers, value)

    def corr_get(phase):
        return get_sum(cb.at[phase], c_send.at[phase], c_recv.at[phase], corr_phases[phase][2])

    ring(0, 1)
    exchange(0)
    send_reflection()
    loads[2].wait()
    flatten(foc_l, into(foc))
    for f in range(2):
        gb[1, f, z, xl] = foc[f].astype(BF)
    ring(0, 2)
    loads[3].wait()
    flatten(res_l, into(fx.at[0, q]))
    for f in range(2):
        share(0, f)
    loads[4].wait()
    ring(0, 3)
    drain(0)
    tables()
    ring(0, 4)
    ring(1, 1)
    exchange(1)
    drain(0)
    assemble_reflection()
    loads[5].wait()

    def square(r, total):
        for f in range(2):
            g = grad_l[f, band(r)]
            total = total + g * g
        return total

    gamma_all = lax.fori_loop(0, ROWS // 8, square, jnp.zeros((8, 2, K), F32))
    gamma_own = added(jnp.sum(gamma_all, axis=0))
    sum_put(0, 0, jnp.broadcast_to(gamma_own, (1, 128)))
    relay(0)
    gathered(0)
    multiply(0, False)
    ring(1, 2)
    for f in range(2):
        fx[1, q, f] = reduced(0, f)
        share(1, f)
    sum_put(0, 1, sum_get(0, 0))
    ring(1, 3)
    shared(0)
    gate_residual()
    relay(1)
    shared(1)
    curvature_own = added(gate_image())
    block_slot = (y * 8 + z) * 2 + xl
    put_sum(bb, b_send, b_recv, block_slot, block_peers, jnp.broadcast_to(curvature_own, (1, 128)))
    gate_again()
    ring(1, 4)
    gamma = sum_get(0, 1)[:, 0:1]
    gathered(1)
    curvature = get_sum(bb, b_send, b_recv, 64)[:, 0:1]
    alpha = gamma / (curvature + TINY)
    for f in range(2):
        gb[2, f, z, xl] = (tr[f] - alpha * ti[f]).astype(BF)
    ring(2, 1)
    exchange(2)
    multiply(1, False)

    def step(r, _):
        rows = band(r)
        for f in range(2):
            v = foc[f, rows, :] + alpha * dirn[f, rows, :]
            o_foc[f, rows, :] = v
            split(s_foc, f, rows, v)
            split(s_res, f, rows, fx[0, q, f, rows, :] - alpha * img[2 * q + f, rows, :])
        return 0

    ring(2, 2)
    lax.fori_loop(0, ROWS // 8, step, 0)
    store(s_foc, foc_out, 0)
    store(s_res, res_out, 1)
    drain(2)
    ring(2, 3)
    for f in range(2):
        fx[2, q, f] = reduced(1, f)
        share(2, f)
    drain(2)
    ring(2, 4)
    drain(2)
    gathered(2)
    multiply(2, True)
    relay(2)
    shared(2)

    def green(r, total):
        rows = band(r)
        fields = fields_of(2, rows)
        out = []
        for e in range(2):
            own = fx[2, q, e, rows, :]
            g = own - gate_own(fields, e, rows)
            g = g + alpha * (fx[1, q, e, rows, :] - img[2 * q + e, rows, :])
            split(s_green, e, rows, g)
            v = o_foc[e, rows, :]
            out += [total[2 * e] + g * v, total[2 * e + 1] + g * swap(v)]
        return tuple(out)

    def finish_corr():
        none = jnp.zeros((8, W), F32)
        sums = lax.fori_loop(0, ROWS // 8, green, (none, none, none, none))
        out = []
        for e in range(2):
            a = jnp.sum(sums[2 * e], axis=0, keepdims=True)
            b = jnp.sum(sums[2 * e + 1], axis=0, keepdims=True)
            out.append(jnp.where(lane[:1] < K, a + swap(a), b - swap(b)))
        return jnp.concatenate(out, axis=0)

    corr_put(0, finish_corr())
    store(s_green, green_out, 2)
    for f in range(2):
        o_dir[f] = reduced(2, f)
    sum_put(1, 0, jnp.broadcast_to(added(squares(lambda e, rows: o_dir[e, rows, :])), (1, 128)))
    corr_put(1, corr_get(0))
    sum_put(1, 1, sum_get(1, 0))
    corr = corr_get(1) * (1.0 / math.sqrt(N))
    for f in range(2):
        o_corr[f, 0:1, :] = corr[f : f + 1, :K]
        o_corr[f, 1:2, :] = corr[f : f + 1, K:]
    store(o_corr, corr_out, 3)
    new_gamma = sum_get(1, 1)[:, 0:1]
    ratio = new_gamma / (gamma + TINY)

    def last(r, _):
        rows = band(r)
        for f in range(2):
            split(s_dir, f, rows, o_dir[f, rows, :] + ratio * dirn[f, rows, :])
        return 0

    lax.fori_loop(0, ROWS // 8, last, 0)
    store(s_dir, dir_out, 4)
    sent(rbuf.at[0:3], r_send)
    for k in range(3):
        sent(gb.at[k, :, 0:7], g_send.at[k])
        sent(gb.at[k, :, 0, 0], x_send.at[k])
        sent(part.at[k, 0:3], s_send.at[k])
        sent(fx.at[k, 0:3], f_send.at[k])
    for d in stores:
        d.wait()


def emit(*refs):
    ins, outs, held, (i_sem, o_sem) = refs[:5], refs[5:10], refs[10:15], refs[15:]
    loads = [pltpu.make_async_copy(ins[i], held[i], i_sem.at[i]) for i in range(5)]
    stores = [pltpu.make_async_copy(held[i], outs[i], o_sem.at[i]) for i in range(5)]
    for d in loads:
        d.start()
    for a, b in zip(loads, stores):
        a.wait()
        b.start()
    for d in stores:
        d.wait()


def per_device(reflection, starts, focusing, residual, direction, gradient):
    field = jax.ShapeDtypeStruct((2, ROWS, 2, K), F32)
    dma = pltpu.SemaphoreType.DMA
    native = pltpu.VMEM((2, ROWS, 2, K), F32)
    flat = pltpu.VMEM((2, ROWS, W), F32)
    hbm = pl.BlockSpec(memory_space=pltpu.HBM)
    shapes = (field, field, field, field, jax.ShapeDtypeStruct((2, 2, K), F32))
    outs = pl.pallas_call(
        kernel,
        out_shape=shapes,
        in_specs=[hbm] * 6,
        out_specs=[hbm] * 5,
        scratch_shapes=[
            pltpu.VMEM((2, 2, ROWS, N), BF),
            pltpu.VMEM((ROWS, K), jnp.int32),
            native, native, native, native, flat, flat,
            flat, flat, native, native, native, native,
            pltpu.VMEM((2, 2, K), F32), dma((6,)), dma((5,)),
            pltpu.VMEM((3, 2, 8, 2, ROWS, W), BF),
            pltpu.VMEM((4, 2, 2, ROWS, COLS), BF),
            pltpu.VMEM((2, 320, COLS), BF),
            pltpu.VMEM((320, COLS), F32),
            pltpu.VMEM((2, COLS, W), F32),
            pltpu.VMEM((320, W), F32),
            pltpu.VMEM((3, 4, 2, ROWS, W), F32),
            pltpu.VMEM((3, 4, 2, ROWS, W), F32),
            pltpu.VMEM((3, 4, 2, ROWS, W), F32),
            pltpu.VMEM((15, ROWS, W), F32),
            pltpu.VMEM((15, ROWS, W), F32),
            pltpu.VMEM((F, ROWS, W), F32),
            pltpu.VMEM((2, ROWS, W), F32),
            pltpu.VMEM((2, ROWS, W), F32),
            pltpu.VMEM((2, 2, 32, 1, 128), F32),
            pltpu.VMEM((2, 32, 2, W), F32),
            dma((3,)), dma((3, 28)), dma((3,)), dma((3,)), dma, dma,
            dma((3,)), dma((3, 2)), dma((3,)), dma((3, 3)),
            dma((2, 2)), dma((2, 2)), dma((2,)), dma((2,)),
            pltpu.VMEM((64, 1, 128), F32), dma, dma,
        ],
        compiler_params=pltpu.CompilerParams(
            collective_id=0, has_side_effects=True, vmem_limit_bytes=63 * 1024 * 1024
        ),
        name="marchenko",
    )(reflection, starts, focusing, residual, direction, gradient)
    return pl.pallas_call(
        emit,
        out_shape=shapes,
        in_specs=[hbm] * 5,
        out_specs=[hbm] * 5,
        scratch_shapes=[
            native, native, native, native, pltpu.VMEM((2, 2, K), F32), dma((5,)), dma((5,)),
        ],
        compiler_params=pltpu.CompilerParams(vmem_limit_bytes=63 * 1024 * 1024),
        name="emit",
    )(*outs)


def solution(mesh):
    finer = Mesh(mesh.devices.reshape(2, 2, 4, 8, 2), AXES)
    field = P(FREQ, RCV, None, None)
    return jax.shard_map(
        per_device,
        mesh=finer,
        in_specs=(P(FREQ, None, RCV, None), P(RCV, None), field, field, field, field),
        out_specs=(field, field, field, field, P(FREQ, None, None)),
        check_vma=False,
    )
```
